32 devices in a mesh: rep: 2 (over x), dp: 4 (over z), sp: 4 (over y, core).
Axes of the slice: x: 2, y: 2, z: 4, core: 2. Of those that a mesh axis runs over, the one named last changes fastest.
Arguments:
- hidden: bfloat16 [256, 3584], P(('rep', 'dp')), parts along dimension 0
- w_query: bfloat16 [3584, 3584], replicated
- w_key: bfloat16 [3584, 512], replicated
- w_value: bfloat16 [3584, 512], replicated
- w_out: bfloat16 [3584, 3584], P('sp')
- k_cache: bfloat16 [256, 1024, 4, 128], P(('rep', 'dp'), 'sp'), parts along dimension 0
- v_cache: bfloat16 [256, 1024, 4, 128], P(('rep', 'dp'), 'sp'), parts along dimension 0
- write_pos: int32 [256], P(('rep', 'dp')), parts along dimension 0
- valid_len: int32 [256], P(('rep', 'dp')), parts along dimension 0
Outputs:
- output 1: bfloat16 [256, 3584], P(('rep', 'dp')), parts along dimension 0
- output 2: bfloat16 [256, 1024, 4, 128], P(('rep', 'dp'), 'sp'), parts along dimension 0
- output 3: bfloat16 [256, 1024, 4, 128], P(('rep', 'dp'), 'sp'), parts along dimension 0
There are 2 independent parts. The reference program is written for one: setup_inputs(seed, part) draws one part's arguments, and reference() takes and returns one part's arrays. A program takes and returns all parts, laid end to end along the dimension named above; an argument that names none is the same for every part.
All inputs are finite; a program needn't handle non-finite values.
Results may differ from the reference program's by a relative error of at most 0.00655233.
Values are sent between devices in bfloat16 or wider.
A program may use at most 1 GiB of HBM per device.

```python
import jax
import jax.numpy as jnp
from jax import lax

MODEL_DIM = 3584
NUM_HEADS = 28
KV_HEADS = 4
HEAD_DIM = 128
BATCH_SIZE = 128
CACHE_LEN = 1024
SEGMENTS = 16


def draw_lengths(rng_key):
    keys = jax.random.split(rng_key, 3)
    shortest = CACHE_LEN // 4
    write_pos = jax.random.randint(keys[0], (BATCH_SIZE,), shortest - 1, CACHE_LEN, jnp.int32)
    long_row = jax.random.randint(keys[1], (), 0, BATCH_SIZE, jnp.int32)
    short_row = (long_row + 1 + jax.random.randint(keys[2], (), 0, BATCH_SIZE - 1, jnp.int32)) % BATCH_SIZE
    row_ids = jnp.arange(BATCH_SIZE, dtype=jnp.int32)
    write_pos = jnp.where(row_ids == long_row, CACHE_LEN - 1, write_pos)
    write_pos = jnp.where(row_ids == short_row, shortest - 1, write_pos)
    return write_pos, write_pos + 1


def setup_inputs(seed: int = 0, part: int = 0) -> dict:
    root = jax.random.key(seed)
    shared = jax.random.split(root, 4)
    own = jax.random.split(jax.random.fold_in(root, part), 8)
    seg_len = CACHE_LEN // SEGMENTS
    proj_width = NUM_HEADS * HEAD_DIM
    kv_width = KV_HEADS * HEAD_DIM
    w_query = (jax.random.normal(shared[0], (MODEL_DIM, proj_width), jnp.float32) * MODEL_DIM ** -0.5).astype(jnp.bfloat16)
    w_key = (jax.random.normal(shared[1], (MODEL_DIM, kv_width), jnp.float32) * MODEL_DIM ** -0.5).astype(jnp.bfloat16)
    w_value = (jax.random.normal(shared[2], (MODEL_DIM, kv_width), jnp.float32) * MODEL_DIM ** -0.5).astype(jnp.bfloat16)
    w_out = (jax.random.normal(shared[3], (proj_width, MODEL_DIM), jnp.float32) * proj_width ** -0.5).astype(jnp.bfloat16)
    hidden = jax.random.normal(own[0], (BATCH_SIZE, MODEL_DIM), jnp.float32).astype(jnp.bfloat16)
    cache_shape = (BATCH_SIZE, SEGMENTS, seg_len, KV_HEADS, HEAD_DIM)
    seg_shape = (BATCH_SIZE, SEGMENTS, 1, KV_HEADS, HEAD_DIM)
    flat_shape = (BATCH_SIZE, CACHE_LEN, KV_HEADS, HEAD_DIM)
    k_cache = (jax.random.normal(own[1], cache_shape, jnp.float32) + jax.random.normal(own[2], seg_shape, jnp.float32)).reshape(flat_shape).astype(jnp.bfloat16)
    v_cache = (jax.random.normal(own[3], cache_shape, jnp.float32) + jax.random.normal(own[4], seg_shape, jnp.float32)).reshape(flat_shape).astype(jnp.bfloat16)
    write_pos, valid_len = draw_lengths(own[5])
    return {'hidden': hidden, 'w_query': w_query, 'w_key': w_key, 'w_value': w_value, 'w_out': w_out, 'k_cache': k_cache, 'v_cache': v_cache, 'write_pos': write_pos, 'valid_len': valid_len}


def reference(hidden, w_query, w_key, w_value, w_out, k_cache, v_cache, write_pos, valid_len):
    group_size = NUM_HEADS // KV_HEADS
    query = jnp.dot(hidden, w_query, preferred_element_type=jnp.float32).astype(jnp.bfloat16)
    query = query.reshape(BATCH_SIZE, KV_HEADS, group_size, HEAD_DIM)
    key_new = jnp.dot(hidden, w_key, preferred_element_type=jnp.float32).astype(jnp.bfloat16)
    value_new = jnp.dot(hidden, w_value, preferred_element_type=jnp.float32).astype(jnp.bfloat16)
    positions = jnp.arange(CACHE_LEN, dtype=jnp.int32)
    at_pos = (positions[None, :] == write_pos[:, None])[:, :, None, None]
    k_next = jnp.where(at_pos, key_new.reshape(BATCH_SIZE, 1, KV_HEADS, HEAD_DIM), k_cache)
    v_next = jnp.where(at_pos, value_new.reshape(BATCH_SIZE, 1, KV_HEADS, HEAD_DIM), v_cache)

    def one_row(row_args):
        q_row, k_row, v_row, length = row_args
        scores = jnp.einsum('kgd,skd->kgs', q_row.astype(jnp.float32), k_row.astype(jnp.float32)) * HEAD_DIM ** -0.5
        scores = jnp.where(positions < length, scores, -jnp.inf)
        row_max = jnp.max(scores, axis=-1, keepdims=True)
        weights = jnp.exp(scores - row_max)
        total = jnp.sum(weights, axis=-1, keepdims=True)
        return jnp.einsum('kgs,skd->kgd', weights, v_row.astype(jnp.float32)) / total

    attention = lax.map(one_row, (query, k_next, v_next, valid_len))
    attention = attention.reshape(BATCH_SIZE, NUM_HEADS * HEAD_DIM).astype(jnp.bfloat16)
    attn_out = jnp.dot(attention, w_out, preferred_element_type=jnp.float32).astype(jnp.bfloat16)
    return (attn_out, k_next, v_next)
```

```python
import jax
import jax.numpy as jnp
from jax import lax
from jax.experimental import pallas as pl
from jax.experimental.pallas import tpu as pltpu
from jax.sharding import PartitionSpec as P

MESH = pl.DeviceIdType.MESH
LOG2E = 1.4426950408889634
NSP = 4
ROWS = 32
DIM = 3584
HEAD = 128
KVH = 4
GRP = 7
SEQ = 256
FLAT = SEQ * KVH
QW = GRP * HEAD
PW = QW + 2 * HEAD
NW = 7
WC = DIM // NW
NB = 4
BC = ROWS // NB
HALF = DIM // 2
NE = 4
NC = 2
CC = HALF // NC


def greet(me):
    barrier = pltpu.get_barrier_semaphore()
    for d in range(1, NSP):
        pl.semaphore_signal(barrier, inc=1, device_id={"sp": lax.rem(me + d, NSP)}, device_id_type=MESH)
    pl.semaphore_wait(barrier, NSP - 1)


def project_kernel(h_ref, wq_ref, wk_ref, wv_ref, kc_ref, vc_ref, qkv_ref, ko_ref, vo_ref,
                   wbuf, acc, mine, recv, wsem, csem, ssem, rsem):
    me = lax.axis_index("sp")
    qcol = pl.multiple_of(me * QW, HEAD)
    kcol = pl.multiple_of(me * HEAD, HEAD)
    copies = []
    for i in range(NW):
        rows = pl.ds(i * WC, WC)
        three = [
            pltpu.make_async_copy(wq_ref.at[rows, pl.ds(qcol, QW)], wbuf.at[rows, pl.ds(0, QW)], wsem.at[i, 0]),
            pltpu.make_async_copy(wk_ref.at[rows, pl.ds(kcol, HEAD)], wbuf.at[rows, pl.ds(QW, HEAD)], wsem.at[i, 1]),
            pltpu.make_async_copy(wv_ref.at[rows, pl.ds(kcol, HEAD)], wbuf.at[rows, pl.ds(QW + HEAD, HEAD)], wsem.at[i, 2]),
        ]
        for c in three:
            c.start()
        copies.append(three)
    caches = []
    for j, (src, dst) in enumerate(((kc_ref, ko_ref), (vc_ref, vo_ref))):
        for i in range(2):
            part = pl.ds(i * (ROWS // 2), ROWS // 2)
            c = pltpu.make_async_copy(src.at[part], dst.at[part], csem.at[j, i])
            c.start()
            caches.append(c)
    greet(me)
    for i in range(NW):
        for c in copies[i]:
            c.wait()
        part = jnp.dot(h_ref[:, i * WC:(i + 1) * WC], wbuf[i * WC:(i + 1) * WC, :], preferred_element_type=jnp.float32)
        if i == 0:
            acc[...] = part
        elif i < NW - 1:
            acc[...] += part
        else:
            mine[...] = (acc[...] + part).astype(jnp.bfloat16)
    sends = []
    for d in range(1, NSP):
        c = pltpu.make_async_remote_copy(
            src_ref=mine, dst_ref=recv.at[d - 1], send_sem=ssem.at[d - 1], recv_sem=rsem.at[d - 1],
            device_id={"sp": lax.rem(me + d, NSP)}, device_id_type=MESH)
        c.start()
        sends.append(c)
    qkv_ref[me] = mine[...]
    for d in range(1, NSP):
        sends[d - 1].wait()
        qkv_ref[lax.rem(me + NSP - d, NSP)] = recv[d - 1]
    for c in caches:
        c.wait()


def export_kernel(pos_ref, qkv_ref, k_in, v_in, ko_ref, vo_ref, k_ref, v_ref, new, sem):
    del k_in, v_in
    base = lax.axis_index("sp") * SEQ
    for j in range(2):
        for r in range(16):
            col = QW + j * HEAD
            new[j, pl.ds(r, ROWS, stride=16), :] = qkv_ref[r % KVH, :, col:col + HEAD].astype(jnp.float32)
    row = lax.broadcasted_iota(jnp.int32, (16, HEAD), 0) // KVH

    def one(b, carry):
        t = pos_ref[b] - base
        inside = jnp.logical_and(t >= 0, t < SEQ)
        tc = jnp.clip(t, 0, SEQ - 1)
        rows = pl.ds(pl.multiple_of((tc // 4) * 16, 16), 16)
        sel = row == jnp.where(inside, tc % 4, -1)
        for j, ref in enumerate((k_ref, v_ref)):
            nb = new[j, pl.ds(pl.multiple_of(b * 16, 16), 16), :]
            ref[b, rows, :] = jnp.where(sel, nb, ref[b, rows, :].astype(jnp.float32)).astype(jnp.bfloat16)
        return carry

    copies = []
    for i in range(NE):
        lax.fori_loop(i * ROWS // NE, (i + 1) * ROWS // NE, one, 0, unroll=4)
        part = pl.ds(i * (ROWS // NE), ROWS // NE)
        for j, (src, dst) in enumerate(((k_ref, ko_ref), (v_ref, vo_ref))):
            c = pltpu.make_async_copy(src.at[part], dst.at[part], sem.at[j, i])
            c.start()
            copies.append(c)
    for c in copies:
        c.wait()


def attend_kernel(len_ref, qkv_ref, k_ref, v_ref, wo_ref, out_ref,
                  qs, kn, vn, mn, cidx, acc, ml, racc, rml, osc, attn, wbuf, part, r1, u, r2, fin, r3,
                  wsem, asem, arsem, msem, mrsem, s1, q1, s2, q2, s3, q3):
    me = lax.axis_index("sp")
    core = lax.rem(me, 2)
    mate = me + 1 - 2 * core
    across = lax.rem(me + 2, NSP)
    wcopies = []
    for i in range(2 * NC):
        cols = pl.ds(i * CC, CC)
        c = pltpu.make_async_copy(wo_ref.at[:, cols], wbuf.at[:, cols], wsem.at[i])
        c.start()
        wcopies.append(c)
    greet(me)
    for g in range(KVH):
        for j in range(8):
            if j < GRP:
                qs[pl.ds(g * 8 + j, ROWS, stride=32), :] = qkv_ref[g, :, j * HEAD:(j + 1) * HEAD].astype(jnp.float32)
            else:
                qs[pl.ds(g * 8 + j, ROWS, stride=32), :] = jnp.zeros((ROWS, HEAD), jnp.float32)
    kn[...] = qkv_ref[me, :, QW:QW + HEAD].astype(jnp.float32)
    vn[...] = qkv_ref[me, :, QW + HEAD:PW].astype(jnp.float32)
    mn[...] = jnp.zeros((8, HEAD), jnp.float32)
    col = lax.broadcasted_iota(jnp.int32, (32, FLAT), 1)
    row = lax.broadcasted_iota(jnp.int32, (32, FLAT), 0)
    cidx[...] = jnp.where(lax.rem(col, KVH) == row // 8, col, 1 << 20)
    ml[:, 0] = jnp.zeros((KVH, 8, HEAD), jnp.float32)
    ml[:, 1] = jnp.ones((KVH, 8, HEAD), jnp.float32)
    lane = lax.broadcasted_iota(jnp.int32, (8, HEAD), 1)
    base = me * SEQ
    factor = HEAD ** -0.5 * LOG2E
    lowest = float(jnp.finfo(jnp.float32).min)

    def pair(p, carry):
        q0 = qs[pl.ds(pl.multiple_of(p * 64, 64), 32), :].astype(jnp.bfloat16)
        q1_ = qs[pl.ds(pl.multiple_of(p * 64 + 32, 32), 32), :].astype(jnp.bfloat16)
        z = jnp.zeros((32, HEAD), jnp.bfloat16)
        lhs = jnp.concatenate([jnp.concatenate([q0, z], 1), jnp.concatenate([z, q1_], 1)], 0)
        kk = jnp.concatenate([k_ref[2 * p], k_ref[2 * p + 1]], 1)
        s = lax.dot_general(lhs, kk, (((1,), (1,)), ((), ())), preferred_element_type=jnp.float32)
        ci = cidx[...]
        ws, ms, ls = [], [], []
        for i in range(2):
            lim = (len_ref[2 * p + i] - 1 - base) * KVH
            si = jnp.where(ci < lim, s[32 * i:32 * (i + 1)], -jnp.inf)
            m = jnp.maximum(jnp.max(si, axis=1, keepdims=True), lowest)
            w = jnp.exp2((si - m) * factor)
            ls.append(jnp.sum(w, axis=1, keepdims=True))
            ms.append(m)
            ws.append(w.astype(jnp.bfloat16))
        vv = jnp.concatenate([v_ref[2 * p], v_ref[2 * p + 1]], 1)
        o = jnp.dot(jnp.concatenate(ws, 0), vv, preferred_element_type=jnp.float32)
        for i in range(2):
            b = 2 * p + i
            here = lane == b
            qb = qs[pl.ds(pl.multiple_of(b * 32 + me * 8, 8), 8), :]
            mn[...] = jnp.where(here, jnp.sum(qb * kn[pl.ds(b, 1), :], axis=1, keepdims=True), mn[...])
            oi = o[32 * i:32 * (i + 1), HEAD * i:HEAD * (i + 1)]
            for g in range(KVH):
                acc[g, b] = oi[8 * g:8 * (g + 1)]
                ml[g, 0] = jnp.where(here, ms[i][8 * g:8 * (g + 1)], ml[g, 0])
                ml[g, 1] = jnp.where(here, ls[i][8 * g:8 * (g + 1)], ml[g, 1])
        return carry

    sends = []
    for cb in range(NB):
        lax.fori_loop(cb * BC // 2, (cb + 1) * BC // 2, pair, 0)
        rows = pl.ds(cb * BC, BC)
        for d in range(1, NSP):
            peer = lax.rem(me + d, NSP)
            c = pltpu.make_async_remote_copy(
                src_ref=acc.at[peer, rows], dst_ref=racc.at[d - 1, rows],
                send_sem=asem.at[d - 1, cb], recv_sem=arsem.at[d - 1, cb],
                device_id={"sp": peer}, device_id_type=MESH)
            c.start()
            sends.append(c)
    for d in range(1, NSP):
        peer = lax.rem(me + d, NSP)
        c = pltpu.make_async_remote_copy(
            src_ref=ml.at[peer], dst_ref=rml.at[d - 1], send_sem=msem.at[d - 1], recv_sem=mrsem.at[d - 1],
            device_id={"sp": peer}, device_id_type=MESH)
        c.start()
        sends.append(c)
    for c in sends:
        c.wait()
    mm = [ml[me, 0]] + [rml[d, 0] for d in range(NSP - 1)]
    ll = [ml[me, 1]] + [rml[d, 1] for d in range(NSP - 1)]
    mm.append(mn[...])
    top = jnp.maximum(jnp.maximum(mm[0], mm[1]), jnp.maximum(jnp.maximum(mm[2], mm[3]), mm[4]))
    ww = [jnp.exp2((m - top) * factor) for m in mm]
    total = ww[0] * ll[0] + ww[1] * ll[1] + ww[2] * ll[2] + ww[3] * ll[3] + ww[4]
    inv = 1.0 / total
    scale = [w * inv for w in ww]
    for b in range(ROWS):
        o = acc[me, b] * scale[0][:, b:b + 1]
        for d in range(NSP - 1):
            o = o + racc[d, b] * scale[d + 1][:, b:b + 1]
        o = o + vn[b:b + 1, :] * scale[NSP][:, b:b + 1]
        osc[pl.ds(b * 8, 8), :] = o
    for j in range(GRP):
        attn[:, j * HEAD:(j + 1) * HEAD] = osc[pl.ds(j, ROWS, stride=8), :].astype(jnp.bfloat16)
    a = attn[...]
    for c in wcopies:
        c.wait()
    c1 = []
    for k in range(NC):
        for other in (1, 0):
            half = lax.rem(core + other, 2)
            cols = pl.ds(pl.multiple_of(half * HALF + k * CC, HEAD), CC)
            part[other, k] = jnp.dot(a, wbuf[:, cols], preferred_element_type=jnp.float32)
            if other:
                c = pltpu.make_async_remote_copy(
                    src_ref=part.at[1, k], dst_ref=r1.at[k], send_sem=s1.at[k], recv_sem=q1.at[k],
                    device_id={"sp": mate}, device_id_type=MESH)
                c.start()
                c1.append(c)
    c2 = []
    for k in range(NC):
        c1[k].wait()
        u[k] = part[0, k] + r1[k]
        c = pltpu.make_async_remote_copy(
            src_ref=u.at[k], dst_ref=r2.at[k], send_sem=s2.at[k], recv_sem=q2.at[k],
            device_id={"sp": across}, device_id_type=MESH)
        c.start()
        c2.append(c)
    c3 = []
    for k in range(NC):
        c2[k].wait()
        fin[k] = (u[k] + r2[k]).astype(jnp.bfloat16)
        c = pltpu.make_async_remote_copy(
            src_ref=fin.at[k], dst_ref=r3.at[k], send_sem=s3.at[k], recv_sem=q3.at[k],
            device_id={"sp": mate}, device_id_type=MESH)
        c.start()
        c3.append(c)
        out_ref[:, pl.ds(pl.multiple_of(core * HALF + k * CC, HEAD), CC)] = fin[k]
    for k in range(NC):
        c3[k].wait()
        out_ref[:, pl.ds(pl.multiple_of((1 - core) * HALF + k * CC, HEAD), CC)] = r3[k]


def solution(mesh):
    row_spec = P(('rep', 'dp'), None)
    cache_spec = P(('rep', 'dp'), 'sp', None, None)
    len_spec = P(('rep', 'dp'))
    hbm = pl.BlockSpec(memory_space=pl.ANY)
    vmem = pl.BlockSpec(memory_space=pltpu.VMEM)
    smem = pl.BlockSpec(memory_space=pltpu.SMEM)
    bf16, f32 = jnp.bfloat16, jnp.float32
    dma = pltpu.SemaphoreType.DMA

    def local_step(hidden, w_query, w_key, w_value, w_out, k_cache, v_cache, write_pos, valid_len):
        kc = k_cache.reshape(ROWS, FLAT, HEAD)
        vc = v_cache.reshape(ROWS, FLAT, HEAD)
        pin = lambda x: pltpu.with_memory_space_constraint(x, pltpu.HBM)
        flat = jax.ShapeDtypeStruct((ROWS, FLAT, HEAD), bf16)
        qkv, kv, vv = pl.pallas_call(
            project_kernel,
            out_shape=[jax.ShapeDtypeStruct((NSP, ROWS, PW), bf16), flat, flat],
            in_specs=[vmem, hbm, hbm, hbm, hbm, hbm],
            out_specs=[vmem, vmem, vmem],
            scratch_shapes=[
                pltpu.VMEM((DIM, PW), bf16), pltpu.VMEM((ROWS, PW), f32), pltpu.VMEM((ROWS, PW), bf16),
                pltpu.VMEM((NSP - 1, ROWS, PW), bf16),
                dma((NW, 3)), dma((2, 2)), dma((NSP - 1,)), dma((NSP - 1,))],
            compiler_params=pltpu.CompilerParams(collective_id=0, has_side_effects=True, vmem_limit_bytes=14 << 20),
            name="project",
            cost_estimate=pl.CostEstimate(flops=10_000_000_000, bytes_accessed=34_000_000, transcendentals=0),
        )(hidden, pin(w_query), pin(w_key), pin(w_value), pin(kc), pin(vc))
        attn_out = pl.pallas_call(
            attend_kernel,
            out_shape=jax.ShapeDtypeStruct((ROWS, DIM), bf16),
            in_specs=[smem, vmem, vmem, vmem, hbm],
            out_specs=vmem,
            scratch_shapes=[
                pltpu.VMEM((ROWS * 32, HEAD), f32), pltpu.VMEM((ROWS, HEAD), f32), pltpu.VMEM((ROWS, HEAD), f32),
                pltpu.VMEM((8, HEAD), f32), pltpu.VMEM((32, FLAT), jnp.int32),
                pltpu.VMEM((KVH, ROWS, 8, HEAD), f32), pltpu.VMEM((KVH, 2, 8, HEAD), f32),
                pltpu.VMEM((NSP - 1, ROWS, 8, HEAD), f32), pltpu.VMEM((NSP - 1, 2, 8, HEAD), f32),
                pltpu.VMEM((ROWS * 8, HEAD), f32), pltpu.VMEM((ROWS, QW), bf16),
                pltpu.VMEM((QW, DIM), bf16),
                pltpu.VMEM((2, NC, ROWS, CC), f32), pltpu.VMEM((NC, ROWS, CC), f32),
                pltpu.VMEM((NC, ROWS, CC), f32), pltpu.VMEM((NC, ROWS, CC), f32),
                pltpu.VMEM((NC, ROWS, CC), bf16), pltpu.VMEM((NC, ROWS, CC), bf16),
                dma((2 * NC,)), dma((NSP - 1, NB)), dma((NSP - 1, NB)), dma((NSP - 1,)), dma((NSP - 1,)),
                dma((NC,)), dma((NC,)), dma((NC,)), dma((NC,)), dma((NC,)), dma((NC,))],
            compiler_params=pltpu.CompilerParams(collective_id=1, has_side_effects=True, vmem_limit_bytes=16 << 20),
            name="attend",
            cost_estimate=pl.CostEstimate(flops=20_000_000_000, bytes_accessed=40_000_000, transcendentals=0),
        )(valid_len, qkv, kv, vv, pin(w_out))
        k_new, v_new, _, _ = pl.pallas_call(
            export_kernel,
            out_shape=[flat, flat, flat, flat],
            in_specs=[smem, vmem, vmem, vmem],
            out_specs=[hbm, hbm, vmem, vmem],
            scratch_shapes=[pltpu.VMEM((2, ROWS * 16, HEAD), f32), dma((2, NE))],
            input_output_aliases={2: 2, 3: 3},
            compiler_params=pltpu.CompilerParams(vmem_limit_bytes=2 << 20),
            name="export",
            cost_estimate=pl.CostEstimate(flops=1_000_000_000, bytes_accessed=34_000_000, transcendentals=0),
        )(write_pos, qkv, kv, vv)
        shape = (ROWS, SEQ, KVH, HEAD)
        return attn_out, k_new.reshape(shape), v_new.reshape(shape)

    return jax.shard_map(local_step, mesh=mesh, in_specs=(row_spec, P(), P(), P(), P('sp', None), cache_spec, cache_spec, len_spec, len_spec), out_specs=(row_spec, cache_spec, cache_spec), check_vma=False)
```

```python
import jax
import jax.numpy as jnp
from jax import lax
from jax.experimental import pallas as pl
from jax.experimental.pallas import tpu as pltpu
from jax.sharding import PartitionSpec as P

MESH = pl.DeviceIdType.MESH
LOG2E = 1.4426950408889634
NSP = 4
ROWS = 32
DIM = 3584
HEAD = 128
KVH = 4
GRP = 7
SEQ = 256
FLAT = SEQ * KVH
QW = GRP * HEAD
PW = QW + 2 * HEAD
NW = 7
WC = DIM // NW
NE = 4
NH = 2
HR = ROWS // NH
HALF = DIM // 2
NC = 1
CC = HALF // NC
FACTOR = HEAD ** -0.5 * LOG2E


def greet(me):
    barrier = pltpu.get_barrier_semaphore()
    for d in range(1, NSP):
        pl.semaphore_signal(barrier, inc=1, device_id={"sp": lax.rem(me + d, NSP)}, device_id_type=MESH)
    pl.semaphore_wait(barrier, NSP - 1)


def project_kernel(h_ref, wq_ref, wk_ref, wv_ref, kc_ref, vc_ref, qkv_ref, ko_ref, vo_ref,
                   wbuf, acc, mine, recv, wsem, csem, ssem, rsem):
    me = lax.axis_index("sp")
    qcol = pl.multiple_of(me * QW, HEAD)
    kcol = pl.multiple_of(me * HEAD, HEAD)
    copies = []
    for i in range(NW):
        rows = pl.ds(i * WC, WC)
        three = [
            pltpu.make_async_copy(wq_ref.at[rows, pl.ds(qcol, QW)], wbuf.at[rows, pl.ds(0, QW)], wsem.at[i, 0]),
            pltpu.make_async_copy(wk_ref.at[rows, pl.ds(kcol, HEAD)], wbuf.at[rows, pl.ds(QW, HEAD)], wsem.at[i, 1]),
            pltpu.make_async_copy(wv_ref.at[rows, pl.ds(kcol, HEAD)], wbuf.at[rows, pl.ds(QW + HEAD, HEAD)], wsem.at[i, 2]),
        ]
        for c in three:
            c.start()
        copies.append(three)
    caches = []
    for j, (src, dst) in enumerate(((kc_ref, ko_ref), (vc_ref, vo_ref))):
        for i in range(2):
            part = pl.ds(i * (ROWS // 2), ROWS // 2)
            c = pltpu.make_async_copy(src.at[part], dst.at[part], csem.at[j, i])
            c.start(priority=1)
            caches.append(c)
    greet(me)
    for i in range(NW):
        for c in copies[i]:
            c.wait()
        part = jnp.dot(h_ref[:, i * WC:(i + 1) * WC], wbuf[i * WC:(i + 1) * WC, :], preferred_element_type=jnp.float32)
        if i == 0:
            acc[...] = part
        elif i < NW - 1:
            acc[...] += part
        else:
            mine[...] = (acc[...] + part).astype(jnp.bfloat16)
    sends = []
    for d in range(1, NSP):
        c = pltpu.make_async_remote_copy(
            src_ref=mine, dst_ref=recv.at[d - 1], send_sem=ssem.at[d - 1], recv_sem=rsem.at[d - 1],
            device_id={"sp": lax.rem(me + d, NSP)}, device_id_type=MESH)
        c.start()
        sends.append(c)
    qkv_ref[me] = mine[...]
    for d in range(1, NSP):
        sends[d - 1].wait()
        qkv_ref[lax.rem(me + NSP - d, NSP)] = recv[d - 1]
    for c in caches:
        c.wait()


def attend_kernel(pos_ref, len_ref, qkv_ref, k_in, v_in, ko_ref, vo_ref, k_ref, v_ref, acc, ml, new, qs, cidx, sem):
    del k_in, v_in
    base = lax.axis_index("sp") * SEQ
    for j in range(2):
        for r in range(16):
            col = QW + j * HEAD
            new[j, pl.ds(r, ROWS, stride=16), :] = qkv_ref[r % KVH, :, col:col + HEAD].astype(jnp.float32)
    row = lax.broadcasted_iota(jnp.int32, (16, HEAD), 0) // KVH

    def patch(b, carry):
        t = pos_ref[b] - base
        inside = jnp.logical_and(t >= 0, t < SEQ)
        tc = jnp.clip(t, 0, SEQ - 1)
        rows = pl.ds(pl.multiple_of((tc // 4) * 16, 16), 16)
        sel = row == jnp.where(inside, tc % 4, -1)
        for j, ref in enumerate((k_ref, v_ref)):
            nb = new[j, pl.ds(pl.multiple_of(b * 16, 16), 16), :]
            ref[b, rows, :] = jnp.where(sel, nb, ref[b, rows, :].astype(jnp.float32)).astype(jnp.bfloat16)
        return carry

    copies = []
    for i in range(NE):
        lax.fori_loop(i * ROWS // NE, (i + 1) * ROWS // NE, patch, 0, unroll=4)
        part = pl.ds(i * (ROWS // NE), ROWS // NE)
        for j, (src, dst) in enumerate(((k_ref, ko_ref), (v_ref, vo_ref))):
            c = pltpu.make_async_copy(src.at[part], dst.at[part], sem.at[j, i])
            c.start()
            copies.append(c)
    for g in range(KVH):
        for j in range(8):
            if j < GRP:
                qs[pl.ds(g * 8 + j, ROWS, stride=32), :] = qkv_ref[g, :, j * HEAD:(j + 1) * HEAD].astype(jnp.float32)
            else:
                qs[pl.ds(g * 8 + j, ROWS, stride=32), :] = jnp.zeros((ROWS, HEAD), jnp.float32)
    col = lax.broadcasted_iota(jnp.int32, (32, FLAT), 1)
    head = lax.broadcasted_iota(jnp.int32, (32, FLAT), 0) // 8
    cidx[...] = jnp.where(lax.rem(col, KVH) == head, col, 1 << 20)
    ml[:, 0] = jnp.zeros((KVH, 8, HEAD), jnp.float32)
    ml[:, 1] = jnp.ones((KVH, 8, HEAD), jnp.float32)
    lane = lax.broadcasted_iota(jnp.int32, (8, HEAD), 1)
    lowest = float(jnp.finfo(jnp.float32).min)

    def pair(p, carry):
        q0 = qs[pl.ds(pl.multiple_of(p * 64, 64), 32), :].astype(jnp.bfloat16)
        q1 = qs[pl.ds(pl.multiple_of(p * 64 + 32, 32), 32), :].astype(jnp.bfloat16)
        z = jnp.zeros((32, HEAD), jnp.bfloat16)
        lhs = jnp.concatenate([jnp.concatenate([q0, z], 1), jnp.concatenate([z, q1], 1)], 0)
        kk = jnp.concatenate([k_ref[2 * p], k_ref[2 * p + 1]], 1)
        s = lax.dot_general(lhs, kk, (((1,), (1,)), ((), ())), preferred_element_type=jnp.float32)
        ci = cidx[...]
        ws, ms, ls = [], [], []
        for i in range(2):
            lim = (len_ref[2 * p + i] - base) * KVH
            si = jnp.where(ci < lim, s[32 * i:32 * (i + 1)], -jnp.inf)
            m = jnp.maximum(jnp.max(si, axis=1, keepdims=True), lowest)
            w = jnp.exp2((si - m) * FACTOR)
            ls.append(jnp.sum(w, axis=1, keepdims=True))
            ms.append(m)
            ws.append(w.astype(jnp.bfloat16))
        vv = jnp.concatenate([v_ref[2 * p], v_ref[2 * p + 1]], 1)
        o = jnp.dot(jnp.concatenate(ws, 0), vv, preferred_element_type=jnp.float32)
        for i in range(2):
            b = 2 * p + i
            here = lane == b
            oi = o[32 * i:32 * (i + 1), HEAD * i:HEAD * (i + 1)]
            for g in range(KVH):
                acc[g, b] = oi[8 * g:8 * (g + 1)]
                ml[g, 0] = jnp.where(here, ms[i][8 * g:8 * (g + 1)], ml[g, 0])
                ml[g, 1] = jnp.where(here, ls[i][8 * g:8 * (g + 1)], ml[g, 1])
        return carry

    lax.fori_loop(0, ROWS // 2, pair, 0, unroll=16)
    for c in copies:
        c.wait()


def combine(parts):
    top = parts[0][0]
    for m, _ in parts[1:]:
        top = jnp.maximum(top, m)
    ww = [jnp.exp2((m - top) * FACTOR) for m, _ in parts]
    total = ww[0] * parts[0][1]
    for w, (_, l) in zip(ww[1:], parts[1:]):
        total = total + w * l
    return top, total, ww


def reduce_kernel(acc, ml, wo_ref, out_ref,
                  ra, rma, cross, mcross, rb, rmb, osc, attn, wbuf, part, r1, u, r2, fin, r3,
                  wsem, sa, qa, sma, qma, sb, qb, smb, qmb, s1, q1, s2, q2, s3, q3):
    me = lax.axis_index("sp")
    core = lax.rem(me, 2)
    mate = me + 1 - 2 * core
    across = lax.rem(me + 2, NSP)
    wcopies = []
    for i in range(4):
        rows = pl.ds(i * (QW // 4), QW // 4)
        c = pltpu.make_async_copy(wo_ref.at[rows], wbuf.at[rows], wsem.at[i])
        c.start(priority=1)
        wcopies.append(c)
    greet(me)

    def send(src, dst, ssem, rsem, peer):
        c = pltpu.make_async_remote_copy(src_ref=src, dst_ref=dst, send_sem=ssem, recv_sem=rsem,
                                         device_id={"sp": peer}, device_id_type=MESH)
        c.start()
        return c

    theirs = (lax.rem(mate + 2, NSP), mate)
    ours = (across, me)
    am = [send(ml.at[theirs[j]], rma.at[j], sma.at[j], qma.at[j], mate) for j in range(2)]
    aa = [[send(acc.at[theirs[j], pl.ds(h * HR, HR)], ra.at[j, pl.ds(h * HR, HR)], sa.at[j, h], qa.at[j, h], mate)
           for h in range(NH)] for j in range(2)]
    am[0].wait()
    top, total, ww = combine([(ml[across, 0], ml[across, 1]), (rma[0, 0], rma[0, 1])])
    mcross[0] = top
    mcross[1] = total
    bm = send(mcross, rmb, smb, qmb, across)
    bb = []
    for h in range(NH):
        aa[0][h].wait()
        for b in range(h * HR, (h + 1) * HR):
            cross[b] = acc[across, b] * ww[0][:, b:b + 1] + ra[0, b] * ww[1][:, b:b + 1]
        rows = pl.ds(h * HR, HR)
        bb.append(send(cross.at[rows], rb.at[rows], sb.at[h], qb.at[h], across))
    am[1].wait()
    bm.wait()
    _, total, ww = combine([(ml[me, 0], ml[me, 1]), (rma[1, 0], rma[1, 1]), (rmb[0], rmb[1])])
    inv = 1.0 / total
    scale = [w * inv for w in ww]
    for h in range(NH):
        aa[1][h].wait()
        for b in range(h * HR, (h + 1) * HR):
            osc[pl.ds(b * 8, 8), :] = acc[me, b] * scale[0][:, b:b + 1] + ra[1, b] * scale[1][:, b:b + 1]
    c1, c2, c3 = {}, {}, {}
    for h in range(NH):
        bb[h].wait()
        for b in range(h * HR, (h + 1) * HR):
            osc[pl.ds(b * 8, 8), :] += rb[b] * scale[2][:, b:b + 1]
        for j in range(GRP):
            attn[h, :, j * HEAD:(j + 1) * HEAD] = osc[pl.ds(h * HR * 8 + j, HR, stride=8), :].astype(jnp.bfloat16)
        a = attn[h]
        if h == 0:
            for c in wcopies:
                c.wait()
        for k in range(NC):
            for other in (1, 0):
                half = lax.rem(core + other, 2)
                cols = pl.ds(pl.multiple_of(half * HALF + k * CC, HEAD), CC)
                part[other, h, k] = jnp.dot(a, wbuf[:, cols], preferred_element_type=jnp.float32)
                if other:
                    c1[h, k] = send(part.at[1, h, k], r1.at[h, k], s1.at[h, k], q1.at[h, k], mate)
        for k in range(NC):
            c1[h, k].wait()
            u[h, k] = part[0, h, k] + r1[h, k]
            c2[h, k] = send(u.at[h, k], r2.at[h, k], s2.at[h, k], q2.at[h, k], across)
    for h in range(NH):
        for k in range(NC):
            c2[h, k].wait()
            fin[h, k] = (u[h, k] + r2[h, k]).astype(jnp.bfloat16)
            c3[h, k] = send(fin.at[h, k], r3.at[h, k], s3.at[h, k], q3.at[h, k], mate)
            out_ref[pl.ds(h * HR, HR), pl.ds(pl.multiple_of(core * HALF + k * CC, HEAD), CC)] = fin[h, k]
    for h in range(NH):
        for k in range(NC):
            c3[h, k].wait()
            out_ref[pl.ds(h * HR, HR), pl.ds(pl.multiple_of((1 - core) * HALF + k * CC, HEAD), CC)] = r3[h, k]


def solution(mesh):
    row_spec = P(('rep', 'dp'), None)
    cache_spec = P(('rep', 'dp'), 'sp', None, None)
    len_spec = P(('rep', 'dp'))
    hbm = pl.BlockSpec(memory_space=pl.ANY)
    vmem = pl.BlockSpec(memory_space=pltpu.VMEM)
    smem = pl.BlockSpec(memory_space=pltpu.SMEM)
    bf16, f32 = jnp.bfloat16, jnp.float32
    dma = pltpu.SemaphoreType.DMA

    def local_step(hidden, w_query, w_key, w_value, w_out, k_cache, v_cache, write_pos, valid_len):
        kc = k_cache.reshape(ROWS, FLAT, HEAD)
        vc = v_cache.reshape(ROWS, FLAT, HEAD)
        pin = lambda x: pltpu.with_memory_space_constraint(x, pltpu.HBM)
        flat = jax.ShapeDtypeStruct((ROWS, FLAT, HEAD), bf16)
        qkv, kv, vv = pl.pallas_call(
            project_kernel,
            out_shape=[jax.ShapeDtypeStruct((NSP, ROWS, PW), bf16), flat, flat],
            in_specs=[vmem, hbm, hbm, hbm, hbm, hbm],
            out_specs=[vmem, vmem, vmem],
            scratch_shapes=[
                pltpu.VMEM((DIM, PW), bf16), pltpu.VMEM((ROWS, PW), f32), pltpu.VMEM((ROWS, PW), bf16),
                pltpu.VMEM((NSP - 1, ROWS, PW), bf16),
                dma((NW, 3)), dma((2, 2)), dma((NSP - 1,)), dma((NSP - 1,))],
            compiler_params=pltpu.CompilerParams(collective_id=0, has_side_effects=True, vmem_limit_bytes=14 << 20),
            name="project",
            cost_estimate=pl.CostEstimate(flops=10_000_000_000, bytes_accessed=34_000_000, transcendentals=0),
        )(hidden, pin(w_query), pin(w_key), pin(w_value), pin(kc), pin(vc))
        tiles = (KVH, ROWS, 8, HEAD)
        k_new, v_new, _, _, acc, ml = pl.pallas_call(
            attend_kernel,
            out_shape=[flat, flat, flat, flat, jax.ShapeDtypeStruct(tiles, f32), jax.ShapeDtypeStruct((KVH, 2, 8, HEAD), f32)],
            in_specs=[smem, smem, vmem, vmem, vmem],
            out_specs=[hbm, hbm, vmem, vmem, vmem, vmem],
            scratch_shapes=[
                pltpu.VMEM((2, ROWS * 16, HEAD), f32), pltpu.VMEM((ROWS * 32, HEAD), f32),
                pltpu.VMEM((32, FLAT), jnp.int32), dma((2, NE))],
            input_output_aliases={3: 2, 4: 3},
            compiler_params=pltpu.CompilerParams(vmem_limit_bytes=6 << 20),
            name="attend",
            cost_estimate=pl.CostEstimate(flops=7_000_000_000, bytes_accessed=34_000_000, transcendentals=0),
        )(write_pos, valid_len, qkv, kv, vv)
        parts = (NH, NC, HR, CC)
        attn_out = pl.pallas_call(
            reduce_kernel,
            out_shape=jax.ShapeDtypeStruct((ROWS, DIM), bf16),
            in_specs=[vmem, vmem, hbm],
            out_specs=vmem,
            scratch_shapes=[
                pltpu.VMEM((2,) + tiles[1:], f32), pltpu.VMEM((2, 2, 8, HEAD), f32),
                pltpu.VMEM(tiles[1:], f32), pltpu.VMEM((2, 8, HEAD), f32),
                pltpu.VMEM(tiles[1:], f32), pltpu.VMEM((2, 8, HEAD), f32),
                pltpu.VMEM((ROWS * 8, HEAD), f32), pltpu.VMEM((NH, HR, QW), bf16), pltpu.VMEM((QW, DIM), bf16),
                pltpu.VMEM((2,) + parts, f32), pltpu.VMEM(parts, f32), pltpu.VMEM(parts, f32), pltpu.VMEM(parts, f32),
                pltpu.VMEM(parts, bf16), pltpu.VMEM(parts, bf16),
                dma((4,)), dma((2, NH)), dma((2, NH)), dma((2,)), dma((2,)), dma((NH,)), dma((NH,)), dma, dma]
                + [dma((NH, NC))] * 6,
            compiler_params=pltpu.CompilerParams(collective_id=1, has_side_effects=True, vmem_limit_bytes=14 << 20),
            name="reduce",
            cost_estimate=pl.CostEstimate(flops=20_000_000_000, bytes_accessed=10_000_000, transcendentals=0),
        )(acc, ml, pin(w_out))
        shape = (ROWS, SEQ, KVH, HEAD)
        return attn_out, k_new.reshape(shape), v_new.reshape(shape)

    return jax.shard_map(local_step, mesh=mesh, in_specs=(row_spec, P(), P(), P(), P('sp', None), cache_spec, cache_spec, len_spec, len_spec), out_specs=(row_spec, cache_spec, cache_spec), check_vma=False)
```

```python
import jax
import jax.numpy as jnp
from jax import lax
from jax.experimental import pallas as pl
from jax.experimental.pallas import tpu as pltpu
from jax.sharding import PartitionSpec as P

MESH = pl.DeviceIdType.MESH
LOG2E = 1.4426950408889634
NSP = 4
ROWS = 32
DIM = 3584
HEAD = 128
KVH = 4
GRP = 7
SEQ = 256
FLAT = SEQ * KVH
QW = GRP * HEAD
PW = QW + 2 * HEAD
PIECES = ((0, 256), (256, 512), (512, 768), (768, QW), (QW, PW))
NP = len(PIECES)
NE = 4
EARLY = 24
LATE = ROWS - EARLY
NH = 2
HR = ROWS // NH
HALF = DIM // 2
NC = 2
CC = HALF // NC
FACTOR = HEAD ** -0.5 * LOG2E
CHUNKS = ((0, HR), (HR, EARLY), (EARLY, ROWS))


def greet(me):
    barrier = pltpu.get_barrier_semaphore()
    for d in range(1, NSP):
        pl.semaphore_signal(barrier, inc=1, device_id={"sp": lax.rem(me + d, NSP)}, device_id_type=MESH)


def greeted():
    pl.semaphore_wait(pltpu.get_barrier_semaphore(), NSP - 1)


def send(src, dst, ssem, rsem, peer):
    c = pltpu.make_async_remote_copy(src_ref=src, dst_ref=dst, send_sem=ssem, recv_sem=rsem,
                                     device_id={"sp": peer}, device_id_type=MESH)
    c.start()
    return c


def project_kernel(h_ref, wq_ref, wk_ref, wv_ref, kc_ref, vc_ref, qs, new, cidx, ko_ref, vo_ref,
                   hbuf, wbuf, mine, recv, hsem, wsem, csem, ssem, rsem):
    me = lax.axis_index("sp")
    mate = me + 1 - 2 * lax.rem(me, 2)
    across = lax.rem(me + 2, NSP)
    qcol = pl.multiple_of(me * QW, HEAD)
    kcol = pl.multiple_of(me * HEAD, HEAD)
    hcopy = pltpu.make_async_copy(h_ref, hbuf, hsem)
    hcopy.start()
    copies = []
    for x, (lo, hi) in enumerate(PIECES):
        if hi <= QW:
            views = [(wq_ref.at[:, pl.ds(pl.multiple_of(qcol + lo, HEAD), hi - lo)], lo)]
        else:
            views = [(wk_ref.at[:, pl.ds(kcol, HEAD)], QW), (wv_ref.at[:, pl.ds(kcol, HEAD)], QW + HEAD)]
        some = []
        for y, (v, at) in enumerate(views):
            c = pltpu.make_async_copy(v, wbuf.at[:, pl.ds(at, v.shape[1])], wsem.at[x, y])
            c.start()
            some.append(c)
        copies.append(some)
    caches = []
    for j, (src, dst) in enumerate(((kc_ref, ko_ref), (vc_ref, vo_ref))):
        for i in range(2):
            part = pl.ds(i * (ROWS // 2), ROWS // 2)
            c = pltpu.make_async_copy(src.at[part], dst.at[part], csem.at[j, i])
            c.start(priority=1)
            caches.append(c)
    greet(me)
    col = lax.broadcasted_iota(jnp.int32, (32, FLAT), 1)
    head = lax.shift_right_logical(lax.broadcasted_iota(jnp.int32, (32, FLAT), 0), 3)
    cidx[...] = jnp.where(lax.bitwise_and(col, KVH - 1) == head, col, 1 << 20)
    for g in range(KVH):
        qs[pl.ds(g * 8 + GRP, ROWS, stride=32), :] = jnp.zeros((ROWS, HEAD), jnp.float32)
    hcopy.wait()
    peers = (across, NSP - 1 - me, mate)
    sends = []
    for x, (lo, hi) in enumerate(PIECES):
        for c in copies[x]:
            c.wait()
        mine[:, lo:hi] = jnp.dot(hbuf[...], wbuf[:, lo:hi], preferred_element_type=jnp.float32).astype(jnp.bfloat16)
        if x == 0:
            greeted()
        cols = pl.ds(lo, hi - lo)
        sends.append([send(mine.at[:, cols], recv.at[y, :, cols], ssem.at[x, y], rsem.at[x, y], peers[y]) for y in range(NSP - 1)])

    def place(g, x, read):
        lo, hi = PIECES[x]
        for at in range(lo, hi, HEAD):
            y = read(at).astype(jnp.float32)
            if at < QW:
                qs[pl.ds(g * 8 + at // HEAD, ROWS, stride=32), :] = y
            else:
                for r in range(4):
                    new[(at - QW) // HEAD, pl.ds(r * KVH + g, ROWS, stride=16), :] = y

    for x in range(NP):
        place(me, x, lambda at: mine[:, at:at + HEAD])
    for x in range(NP):
        for y in (2, 0, 1):
            sends[x][y].wait()
            place(peers[y], x, lambda at: recv[y, :, at:at + HEAD])
    for c in caches:
        c.wait()


def attention(first, count, unroll, rows0, len_ref, qs, cidx, k_ref, v_ref, acc, ml):
    base = lax.axis_index("sp") * SEQ
    lane = lax.broadcasted_iota(jnp.int32, (8, HEAD), 1)
    lowest = float(jnp.finfo(jnp.float32).min)

    def pair(p, carry):
        q0 = qs[pl.ds(pl.multiple_of(p * 64, 64), 32), :].astype(jnp.bfloat16)
        q1 = qs[pl.ds(pl.multiple_of(p * 64 + 32, 32), 32), :].astype(jnp.bfloat16)
        z = jnp.zeros((32, HEAD), jnp.bfloat16)
        lhs = jnp.concatenate([jnp.concatenate([q0, z], 1), jnp.concatenate([z, q1], 1)], 0)
        kk = jnp.concatenate([k_ref[2 * p], k_ref[2 * p + 1]], 1)
        s = lax.dot_general(lhs, kk, (((1,), (1,)), ((), ())), preferred_element_type=jnp.float32)
        ci = cidx[...]
        ws, ms, ls = [], [], []
        for i in range(2):
            lim = (len_ref[2 * p + i] - base) * KVH
            si = jnp.where(ci < lim, s[32 * i:32 * (i + 1)], -jnp.inf)
            m = jnp.maximum(jnp.max(si, axis=1, keepdims=True), lowest)
            w = jnp.exp2((si - m) * FACTOR)
            ls.append(jnp.sum(w, axis=1, keepdims=True))
            ms.append(m)
            ws.append(w.astype(jnp.bfloat16))
        vv = jnp.concatenate([v_ref[2 * p], v_ref[2 * p + 1]], 1)
        o = jnp.dot(jnp.concatenate(ws, 0), vv, preferred_element_type=jnp.float32)
        for i in range(2):
            b = 2 * p + i
            here = lane == b
            oi = o[32 * i:32 * (i + 1), HEAD * i:HEAD * (i + 1)]
            for g in range(KVH):
                acc[g, b - rows0] = oi[8 * g:8 * (g + 1)]
                ml[g, 0] = jnp.where(here, ms[i][8 * g:8 * (g + 1)], ml[g, 0])
                ml[g, 1] = jnp.where(here, ls[i][8 * g:8 * (g + 1)], ml[g, 1])
        return carry

    lax.fori_loop(first // 2, (first + count) // 2, pair, 0, unroll=unroll)


def attend_kernel(pos_ref, len_ref, qs, new, cidx, k_in, v_in, ko_ref, vo_ref, k_ref, v_ref, acc, ml, sem):
    del k_in, v_in
    base = lax.axis_index("sp") * SEQ
    row = lax.shift_right_logical(lax.broadcasted_iota(jnp.int32, (16, HEAD), 0), 2)

    def patch(b, carry):
        t = pos_ref[b] - base
        inside = jnp.logical_and(t >= 0, t < SEQ)
        tc = jnp.clip(t, 0, SEQ - 1)
        rows = pl.ds(pl.multiple_of(lax.shift_right_logical(tc, 2) * 16, 16), 16)
        sel = row == jnp.where(inside, lax.bitwise_and(tc, 3), -1)
        for j, ref in enumerate((k_ref, v_ref)):
            nb = new[j, pl.ds(pl.multiple_of(b * 16, 16), 16), :]
            ref[b, rows, :] = jnp.where(sel, nb, ref[b, rows, :].astype(jnp.float32)).astype(jnp.bfloat16)
        return carry

    copies = []
    for i in range(NE):
        lax.fori_loop(i * ROWS // NE, (i + 1) * ROWS // NE, patch, 0, unroll=8)
        part = pl.ds(i * (ROWS // NE), ROWS // NE)
        for j, (src, dst) in enumerate(((k_ref, ko_ref), (v_ref, vo_ref))):
            c = pltpu.make_async_copy(src.at[part], dst.at[part], sem.at[j, i])
            c.start()
            copies.append(c)
    ml[:, 0] = jnp.zeros((KVH, 8, HEAD), jnp.float32)
    ml[:, 1] = jnp.ones((KVH, 8, HEAD), jnp.float32)
    attention(0, EARLY, EARLY // 2, 0, len_ref, qs, cidx, k_ref, v_ref, acc, ml)
    for c in copies:
        c.wait()


def combine(parts):
    top = parts[0][0]
    for m, _ in parts[1:]:
        top = jnp.maximum(top, m)
    ww = [jnp.exp2((m - top) * FACTOR) for m, _ in parts]
    total = ww[0] * parts[0][1]
    for w, (_, l) in zip(ww[1:], parts[1:]):
        total = total + w * l
    return top, total, ww


def reduce_kernel(len_ref, qs, cidx, k_ref, v_ref, acc0, ml0, wo_ref, out_ref,
                  acc1, ml1, ra, rma, cross, mcross, rb, rmb, osc, attn, wbuf, part, r1, u, r2, fin, r3,
                  wsem, sa, qa, sma, qma, sb, qb, smb, qmb, s1, q1, s2, q2, s3, q3):
    me = lax.axis_index("sp")
    core = lax.rem(me, 2)
    mate = me + 1 - 2 * core
    across = lax.rem(me + 2, NSP)
    greet(me)
    wcopies = []
    for i in range(4):
        rows = pl.ds(i * (QW // 4), QW // 4)
        c = pltpu.make_async_copy(wo_ref.at[rows], wbuf.at[rows], wsem.at[i])
        c.start(priority=1)
        wcopies.append(c)
    ml1[:, 0] = jnp.zeros((KVH, 8, HEAD), jnp.float32)
    ml1[:, 1] = jnp.ones((KVH, 8, HEAD), jnp.float32)
    attention(EARLY, LATE // 2, LATE // 4, EARLY, len_ref, qs, cidx, k_ref, v_ref, acc1, ml1)
    greeted()

    theirs = (lax.rem(mate + 2, NSP), mate)
    mls = (ml0, ml1)
    accs = (acc0, acc1)
    starts = (0, EARLY)
    am, aa = {}, {}

    def to_mate(p, j, chunks):
        am[p, j] = send(mls[p].at[theirs[j]], rma.at[p, j], sma.at[p, j], qma.at[p, j], mate)
        for x in chunks:
            lo, hi = CHUNKS[x]
            aa[x, j] = send(accs[p].at[theirs[j], pl.ds(lo - starts[p], hi - lo)], ra.at[j, pl.ds(lo, hi - lo)],
                            sa.at[x, j], qa.at[x, j], mate)

    to_mate(0, 0, (0, 1))
    to_mate(0, 1, (0, 1))
    attention(EARLY + LATE // 2, LATE // 2, LATE // 4, EARLY, len_ref, qs, cidx, k_ref, v_ref, acc1, ml1)
    to_mate(1, 0, (2,))
    to_mate(1, 1, (2,))
    bm, bb = {}, {}
    for p in range(2):
        am[p, 0].wait()
        top, total, ww = combine([(mls[p][across, 0], mls[p][across, 1]), (rma[p, 0, 0], rma[p, 0, 1])])
        mcross[p, 0] = top
        mcross[p, 1] = total
        bm[p] = send(mcross.at[p], rmb.at[p], smb.at[p], qmb.at[p], across)
        for x in ((0, 1), (2,))[p]:
            lo, hi = CHUNKS[x]
            aa[x, 0].wait()
            for b in range(lo, hi):
                cross[b] = accs[p][across, b - starts[p]] * ww[0][:, b:b + 1] + ra[0, b] * ww[1][:, b:b + 1]
            rows = pl.ds(lo, hi - lo)
            bb[x] = send(cross.at[rows], rb.at[rows], sb.at[x], qb.at[x], across)
    scales = {}

    def own(p, chunks):
        if p not in scales:
            am[p, 1].wait()
            bm[p].wait()
            _, total, ww = combine([(mls[p][me, 0], mls[p][me, 1]), (rma[p, 1, 0], rma[p, 1, 1]), (rmb[p, 0], rmb[p, 1])])
            inv = 1.0 / total
            scales[p] = [w * inv for w in ww]
        scale = scales[p]
        for x in chunks:
            aa[x, 1].wait()
            bb[x].wait()
            for b in range(*CHUNKS[x]):
                osc[pl.ds(b * 8, 8), :] = (accs[p][me, b - starts[p]] * scale[0][:, b:b + 1] + ra[1, b] * scale[1][:, b:b + 1]
                                           + rb[b] * scale[2][:, b:b + 1])

    def gathered(h):
        for j in range(GRP):
            attn[h, :, j * HEAD:(j + 1) * HEAD] = osc[pl.ds(h * HR * 8 + j, HR, stride=8), :].astype(jnp.bfloat16)

    c1, c2, c3 = {}, {}, {}

    def multiply(h):
        a = attn[h]
        for k in range(NC):
            for other in (1, 0):
                half = lax.rem(core + other, 2)
                cols = pl.ds(pl.multiple_of(half * HALF + k * CC, HEAD), CC)
                part[other, h, k] = jnp.dot(a, wbuf[:, cols], preferred_element_type=jnp.float32)
                if other:
                    c1[h, k] = send(part.at[1, h, k], r1.at[h, k], s1.at[h, k], q1.at[h, k], mate)

    def pass_on(h):
        for k in range(NC):
            c1[h, k].wait()
            u[h, k] = part[0, h, k] + r1[h, k]
            c2[h, k] = send(u.at[h, k], r2.at[h, k], s2.at[h, k], q2.at[h, k], across)

    own(0, (0,))
    gathered(0)
    for c in wcopies:
        c.wait()
    multiply(0)
    own(0, (1,))
    own(1, (2,))
    gathered(1)
    pass_on(0)
    multiply(1)
    pass_on(1)
    for h in range(NH):
        for k in range(NC):
            c2[h, k].wait()
            fin[h, k] = (u[h, k] + r2[h, k]).astype(jnp.bfloat16)
            c3[h, k] = send(fin.at[h, k], r3.at[h, k], s3.at[h, k], q3.at[h, k], mate)
            out_ref[pl.ds(h * HR, HR), pl.ds(pl.multiple_of(core * HALF + k * CC, HEAD), CC)] = fin[h, k]
    for h in range(NH):
        for k in range(NC):
            c3[h, k].wait()
            out_ref[pl.ds(h * HR, HR), pl.ds(pl.multiple_of((1 - core) * HALF + k * CC, HEAD), CC)] = r3[h, k]


def solution(mesh):
    row_spec = P(('rep', 'dp'), None)
    cache_spec = P(('rep', 'dp'), 'sp', None, None)
    len_spec = P(('rep', 'dp'))
    hbm = pl.BlockSpec(memory_space=pl.ANY)
    vmem = pl.BlockSpec(memory_space=pltpu.VMEM)
    smem = pl.BlockSpec(memory_space=pltpu.SMEM)
    bf16, f32, i32 = jnp.bfloat16, jnp.float32, jnp.int32
    dma = pltpu.SemaphoreType.DMA
    shaped = jax.ShapeDtypeStruct

    def local_step(hidden, w_query, w_key, w_value, w_out, k_cache, v_cache, write_pos, valid_len):
        kc = k_cache.reshape(ROWS, FLAT, HEAD)
        vc = v_cache.reshape(ROWS, FLAT, HEAD)
        pin = lambda x: pltpu.with_memory_space_constraint(x, pltpu.HBM)
        flat = shaped((ROWS, FLAT, HEAD), bf16)
        qs, new, cidx, kv, vv = pl.pallas_call(
            project_kernel,
            out_shape=[shaped((ROWS * 32, HEAD), f32), shaped((2, ROWS * 16, HEAD), f32), shaped((32, FLAT), i32), flat, flat],
            in_specs=[hbm] * 6,
            out_specs=[vmem] * 5,
            scratch_shapes=[
                pltpu.VMEM((ROWS, DIM), bf16), pltpu.VMEM((DIM, PW), bf16),
                pltpu.VMEM((ROWS, PW), bf16), pltpu.VMEM((NSP - 1, ROWS, PW), bf16),
                dma, dma((NP, 2)), dma((2, 2)), dma((NP, NSP - 1)), dma((NP, NSP - 1))],
            compiler_params=pltpu.CompilerParams(collective_id=0, has_side_effects=True, vmem_limit_bytes=14 << 20),
            name="project",
            cost_estimate=pl.CostEstimate(flops=10_000_000_000, bytes_accessed=34_000_000, transcendentals=0),
        )(pin(hidden), pin(w_query), pin(w_key), pin(w_value), pin(kc), pin(vc))
        tiles = (8, HEAD)
        k_new, v_new, kv, vv, acc, ml = pl.pallas_call(
            attend_kernel,
            out_shape=[flat, flat, flat, flat, shaped((KVH, EARLY) + tiles, f32), shaped((KVH, 2) + tiles, f32)],
            in_specs=[smem, smem] + [vmem] * 5,
            out_specs=[hbm, hbm, vmem, vmem, vmem, vmem],
            scratch_shapes=[dma((2, NE))],
            input_output_aliases={5: 2, 6: 3},
            compiler_params=pltpu.CompilerParams(vmem_limit_bytes=4 << 20),
            name="attend",
            cost_estimate=pl.CostEstimate(flops=7_000_000_000, bytes_accessed=34_000_000, transcendentals=0),
        )(write_pos, valid_len, qs, new, cidx, kv, vv)
        parts = (NH, NC, HR, CC)
        nx = len(CHUNKS)
        attn_out = pl.pallas_call(
            reduce_kernel,
            out_shape=shaped((ROWS, DIM), bf16),
            in_specs=[smem] + [vmem] * 6 + [hbm],
            out_specs=vmem,
            scratch_shapes=[
                pltpu.VMEM((KVH, LATE) + tiles, f32), pltpu.VMEM((KVH, 2) + tiles, f32),
                pltpu.VMEM((2, ROWS) + tiles, f32), pltpu.VMEM((2, 2, 2) + tiles, f32),
                pltpu.VMEM((ROWS,) + tiles, f32), pltpu.VMEM((2, 2) + tiles, f32),
                pltpu.VMEM((ROWS,) + tiles, f32), pltpu.VMEM((2, 2) + tiles, f32),
                pltpu.VMEM((ROWS * 8, HEAD), f32), pltpu.VMEM((NH, HR, QW), bf16), pltpu.VMEM((QW, DIM), bf16),
                pltpu.VMEM((2,) + parts, f32), pltpu.VMEM(parts, f32), pltpu.VMEM(parts, f32), pltpu.VMEM(parts, f32),
                pltpu.VMEM(parts, bf16), pltpu.VMEM(parts, bf16),
                dma((4,)), dma((nx, 2)), dma((nx, 2)), dma((2, 2)), dma((2, 2)), dma((nx,)), dma((nx,)), dma((2,)), dma((2,))]
                + [dma((NH, NC))] * 6,
            compiler_params=pltpu.CompilerParams(collective_id=1, has_side_effects=True, vmem_limit_bytes=14 << 20),
            name="reduce",
            cost_estimate=pl.CostEstimate(flops=20_000_000_000, bytes_accessed=10_000_000, transcendentals=0),
        )(valid_len, qs, cidx, kv, vv, acc, ml, pin(w_out))
        shape = (ROWS, SEQ, KVH, HEAD)
        return attn_out, k_new.reshape(shape), v_new.reshape(shape)

    return jax.shard_map(local_step, mesh=mesh, in_specs=(row_spec, P(), P(), P(), P('sp', None), cache_spec, cache_spec, len_spec, len_spec), out_specs=(row_spec, cache_spec, cache_spec), check_vma=False)
```

```python
import jax
import jax.numpy as jnp
from jax import lax
from jax.experimental import pallas as pl
from jax.experimental.pallas import tpu as pltpu
from jax.sharding import PartitionSpec as P

MESH = pl.DeviceIdType.MESH
LOG2E = 1.4426950408889634
NSP = 4
ROWS = 32
DIM = 3584
HEAD = 128
KVH = 4
GRP = 7
SEQ = 256
FLAT = SEQ * KVH
QW = GRP * HEAD
PW = QW + 2 * HEAD
PIECES = ((0, 256), (256, 512), (512, 768), (768, QW), (QW, PW))
NP = len(PIECES)
OUT = (0, 8, 16, 24, 28, ROWS)
NE = len(OUT) - 1
EARLY = 24
LATE = ROWS - EARLY
NH = 2
HR = ROWS // NH
HALF = DIM // 2
CUTS = ((0, 512), (512, 1280), (1280, HALF))
NC = len(CUTS)
LAST = (NH - 1, NC - 1)
FACTOR = HEAD ** -0.5 * LOG2E
CHUNKS = ((0, HR), (HR, EARLY), (EARLY, ROWS))


def greet(me):
    barrier = pltpu.get_barrier_semaphore()
    for d in range(1, NSP):
        pl.semaphore_signal(barrier, inc=1, device_id={"sp": lax.rem(me + d, NSP)}, device_id_type=MESH)


def greeted():
    pl.semaphore_wait(pltpu.get_barrier_semaphore(), NSP - 1)


def send(src, dst, ssem, rsem, peer):
    c = pltpu.make_async_remote_copy(src_ref=src, dst_ref=dst, send_sem=ssem, recv_sem=rsem,
                                     device_id={"sp": peer}, device_id_type=MESH)
    c.start()
    return c


def project_kernel(h_ref, wq_ref, wk_ref, wv_ref, kc_ref, vc_ref, qs, new, cidx, ko_ref, vo_ref,
                   hbuf, wbuf, mine, recv, hsem, wsem, csem, ssem, rsem):
    me = lax.axis_index("sp")
    mate = me + 1 - 2 * lax.rem(me, 2)
    across = lax.rem(me + 2, NSP)
    qcol = pl.multiple_of(me * QW, HEAD)
    kcol = pl.multiple_of(me * HEAD, HEAD)
    hcopy = pltpu.make_async_copy(h_ref, hbuf, hsem)
    hcopy.start()
    copies = []
    for x, (lo, hi) in enumerate(PIECES):
        if hi <= QW:
            views = [(wq_ref.at[:, pl.ds(pl.multiple_of(qcol + lo, HEAD), hi - lo)], lo)]
        else:
            views = [(wk_ref.at[:, pl.ds(kcol, HEAD)], QW), (wv_ref.at[:, pl.ds(kcol, HEAD)], QW + HEAD)]
        some = []
        for y, (v, at) in enumerate(views):
            c = pltpu.make_async_copy(v, wbuf.at[:, pl.ds(at, v.shape[1])], wsem.at[x, y])
            c.start()
            some.append(c)
        copies.append(some)
    caches = []
    for j, (src, dst) in enumerate(((kc_ref, ko_ref), (vc_ref, vo_ref))):
        for i in range(2):
            part = pl.ds(i * (ROWS // 2), ROWS // 2)
            c = pltpu.make_async_copy(src.at[part], dst.at[part], csem.at[j, i])
            c.start(priority=1)
            caches.append(c)
    greet(me)
    col = lax.broadcasted_iota(jnp.int32, (32, FLAT), 1)
    head = lax.shift_right_logical(lax.broadcasted_iota(jnp.int32, (32, FLAT), 0), 3)
    cidx[...] = jnp.where(lax.bitwise_and(col, KVH - 1) == head, col, 1 << 20)
    for g in range(KVH):
        qs[pl.ds(g * 8 + GRP, ROWS, stride=32), :] = jnp.zeros((ROWS, HEAD), jnp.float32)
    hcopy.wait()
    peers = (across, NSP - 1 - me, mate)
    sends = []
    for x, (lo, hi) in enumerate(PIECES):
        for c in copies[x]:
            c.wait()
        mine[:, lo:hi] = jnp.dot(hbuf[...], wbuf[:, lo:hi], preferred_element_type=jnp.float32).astype(jnp.bfloat16)
        if x == 0:
            greeted()
        cols = pl.ds(lo, hi - lo)
        sends.append([send(mine.at[:, cols], recv.at[y, :, cols], ssem.at[x, y], rsem.at[x, y], peers[y]) for y in range(NSP - 1)])

    def place(g, x, read):
        lo, hi = PIECES[x]
        for at in range(lo, hi, HEAD):
            y = read(at).astype(jnp.float32)
            if at < QW:
                qs[pl.ds(g * 8 + at // HEAD, ROWS, stride=32), :] = y
            else:
                for r in range(4):
                    new[(at - QW) // HEAD, pl.ds(r * KVH + g, ROWS, stride=16), :] = y

    for x in range(NP):
        place(me, x, lambda at: mine[:, at:at + HEAD])
    for x in range(NP):
        for y in (2, 0, 1):
            sends[x][y].wait()
            place(peers[y], x, lambda at: recv[y, :, at:at + HEAD])
    for c in caches:
        c.wait()


def attention(first, count, unroll, rows0, len_ref, qs, cidx, k_ref, v_ref, acc, ml):
    base = lax.axis_index("sp") * SEQ
    lane = lax.broadcasted_iota(jnp.int32, (8, HEAD), 1)
    lowest = float(jnp.finfo(jnp.float32).min)

    def pair(p, carry):
        q0 = qs[pl.ds(pl.multiple_of(p * 64, 64), 32), :].astype(jnp.bfloat16)
        q1 = qs[pl.ds(pl.multiple_of(p * 64 + 32, 32), 32), :].astype(jnp.bfloat16)
        z = jnp.zeros((32, HEAD), jnp.bfloat16)
        lhs = jnp.concatenate([jnp.concatenate([q0, z], 1), jnp.concatenate([z, q1], 1)], 0)
        kk = jnp.concatenate([k_ref[2 * p], k_ref[2 * p + 1]], 1)
        s = lax.dot_general(lhs, kk, (((1,), (1,)), ((), ())), preferred_element_type=jnp.float32)
        ci = cidx[...]
        ws, ms, ls = [], [], []
        for i in range(2):
            lim = (len_ref[2 * p + i] - base) * KVH
            si = jnp.where(ci < lim, s[32 * i:32 * (i + 1)], -jnp.inf)
            m = jnp.maximum(jnp.max(si, axis=1, keepdims=True), lowest)
            w = jnp.exp2((si - m) * FACTOR)
            ls.append(jnp.sum(w, axis=1, keepdims=True))
            ms.append(m)
            ws.append(w.astype(jnp.bfloat16))
        vv = jnp.concatenate([v_ref[2 * p], v_ref[2 * p + 1]], 1)
        o = jnp.dot(jnp.concatenate(ws, 0), vv, preferred_element_type=jnp.float32)
        for i in range(2):
            b = 2 * p + i
            here = lane == b
            oi = o[32 * i:32 * (i + 1), HEAD * i:HEAD * (i + 1)]
            for g in range(KVH):
                acc[g, b - rows0] = oi[8 * g:8 * (g + 1)]
                ml[g, 0] = jnp.where(here, ms[i][8 * g:8 * (g + 1)], ml[g, 0])
                ml[g, 1] = jnp.where(here, ls[i][8 * g:8 * (g + 1)], ml[g, 1])
        return carry

    lax.fori_loop(first // 2, (first + count) // 2, pair, 0, unroll=unroll)


def attend_kernel(pos_ref, len_ref, qs, new, cidx, k_in, v_in, ko_ref, vo_ref, k_ref, v_ref, acc, ml, sem):
    del k_in, v_in
    base = lax.axis_index("sp") * SEQ
    row = lax.shift_right_logical(lax.broadcasted_iota(jnp.int32, (16, HEAD), 0), 2)

    def patch(first, last):
        todo = []
        for b in range(first, last):
            t = pos_ref[b] - base
            inside = jnp.logical_and(t >= 0, t < SEQ)
            tc = jnp.clip(t, 0, SEQ - 1)
            rows = pl.ds(pl.multiple_of(lax.shift_right_logical(tc, 2) * 16, 16), 16)
            sel = row == jnp.where(inside, lax.bitwise_and(tc, 3), -1)
            for j, ref in enumerate((k_ref, v_ref)):
                old = ref[b, rows, :].astype(jnp.float32)
                todo.append((ref, b, rows, jnp.where(sel, new[j, b * 16:(b + 1) * 16, :], old).astype(jnp.bfloat16)))
        for ref, b, rows, x in todo:
            ref[b, rows, :] = x

    copies = []
    for i in range(NE):
        lo, hi = OUT[i], OUT[i + 1]
        for b in range(lo, hi, 4):
            patch(b, b + 4)
        part = pl.ds(lo, hi - lo)
        for j, (src, dst) in enumerate(((k_ref, ko_ref), (v_ref, vo_ref))):
            c = pltpu.make_async_copy(src.at[part], dst.at[part], sem.at[j, i])
            c.start()
            copies.append(c)
    ml[:, 0] = jnp.zeros((KVH, 8, HEAD), jnp.float32)
    ml[:, 1] = jnp.ones((KVH, 8, HEAD), jnp.float32)
    attention(0, EARLY, EARLY // 2, 0, len_ref, qs, cidx, k_ref, v_ref, acc, ml)
    for c in copies:
        c.wait()


def combine(parts):
    top = parts[0][0]
    for m, _ in parts[1:]:
        top = jnp.maximum(top, m)
    ww = [jnp.exp2((m - top) * FACTOR) for m, _ in parts]
    total = ww[0] * parts[0][1]
    for w, (_, l) in zip(ww[1:], parts[1:]):
        total = total + w * l
    return top, total, ww


def reduce_kernel(len_ref, qs, cidx, k_ref, v_ref, acc0, ml0, wo_ref, out_ref,
                  acc1, ml1, ra, rma, cross, mcross, rb, rmb, osc, attn, wbuf, part, r1, u, r2, fin, r3,
                  wsem, sa, qa, sma, qma, sb, qb, smb, qmb, s1, q1, s2, q2, s3, q3, v1, v2, sv, qv):
    me = lax.axis_index("sp")
    core = lax.rem(me, 2)
    mate = me + 1 - 2 * core
    across = lax.rem(me + 2, NSP)
    greet(me)
    wcopies = []
    for i in range(4):
        rows = pl.ds(i * (QW // 4), QW // 4)
        c = pltpu.make_async_copy(wo_ref.at[rows], wbuf.at[rows], wsem.at[i])
        c.start(priority=1)
        wcopies.append(c)
    ml1[:, 0] = jnp.zeros((KVH, 8, HEAD), jnp.float32)
    ml1[:, 1] = jnp.ones((KVH, 8, HEAD), jnp.float32)
    attention(EARLY, LATE // 2, LATE // 4, EARLY, len_ref, qs, cidx, k_ref, v_ref, acc1, ml1)
    greeted()

    theirs = (lax.rem(mate + 2, NSP), mate)
    mls = (ml0, ml1)
    accs = (acc0, acc1)
    starts = (0, EARLY)
    am, aa = {}, {}

    def to_mate(p, j, chunks):
        am[p, j] = send(mls[p].at[theirs[j]], rma.at[p, j], sma.at[p, j], qma.at[p, j], mate)
        for x in chunks:
            lo, hi = CHUNKS[x]
            aa[x, j] = send(accs[p].at[theirs[j], pl.ds(lo - starts[p], hi - lo)], ra.at[j, pl.ds(lo, hi - lo)],
                            sa.at[x, j], qa.at[x, j], mate)

    to_mate(0, 0, (0, 1))
    to_mate(0, 1, (0, 1))
    attention(EARLY + LATE // 2, LATE // 2, LATE // 4, EARLY, len_ref, qs, cidx, k_ref, v_ref, acc1, ml1)
    to_mate(1, 0, (2,))
    to_mate(1, 1, (2,))
    bm, bb = {}, {}
    for p in range(2):
        am[p, 0].wait()
        top, total, ww = combine([(mls[p][across, 0], mls[p][across, 1]), (rma[p, 0, 0], rma[p, 0, 1])])
        mcross[p, 0] = top
        mcross[p, 1] = total
        bm[p] = send(mcross.at[p], rmb.at[p], smb.at[p], qmb.at[p], across)
        for x in ((0, 1), (2,))[p]:
            lo, hi = CHUNKS[x]
            aa[x, 0].wait()
            for b in range(lo, hi):
                cross[b] = accs[p][across, b - starts[p]] * ww[0][:, b:b + 1] + ra[0, b] * ww[1][:, b:b + 1]
            rows = pl.ds(lo, hi - lo)
            bb[x] = send(cross.at[rows], rb.at[rows], sb.at[x], qb.at[x], across)
    scales = {}

    def own(p, chunks):
        if p not in scales:
            am[p, 1].wait()
            bm[p].wait()
            _, total, ww = combine([(mls[p][me, 0], mls[p][me, 1]), (rma[p, 1, 0], rma[p, 1, 1]), (rmb[p, 0], rmb[p, 1])])
            inv = 1.0 / total
            scales[p] = [w * inv for w in ww]
        scale = scales[p]
        for x in chunks:
            aa[x, 1].wait()
            for b in range(*CHUNKS[x]):
                osc[pl.ds(b * 8, 8), :] = accs[p][me, b - starts[p]] * scale[0][:, b:b + 1] + ra[1, b] * scale[1][:, b:b + 1]

    def far(p, chunks):
        for x in chunks:
            bb[x].wait()
            for b in range(*CHUNKS[x]):
                osc[pl.ds(b * 8, 8), :] += rb[b] * scales[p][2][:, b:b + 1]

    def gathered(h):
        for j in range(GRP):
            attn[h, :, j * HEAD:(j + 1) * HEAD] = osc[pl.ds(h * HR * 8 + j, HR, stride=8), :].astype(jnp.bfloat16)

    c1, c2, c3, direct = {}, {}, {}, []
    rows_of = lambda h: pl.ds(h * HR, HR)

    def multiply(h, k, other):
        lo, hi = CUTS[k]
        half = lax.rem(core + other, 2)
        cols = pl.ds(pl.multiple_of(half * HALF + lo, HEAD), hi - lo)
        part[other, h, :, lo:hi] = jnp.dot(attn[h], wbuf[:, cols], preferred_element_type=jnp.float32)

    def product(h):
        for k, (lo, hi) in enumerate(CUTS):
            multiply(h, k, 1)
            cols = pl.ds(lo, hi - lo)
            c1[h, k] = send(part.at[1, h, :, cols], r1.at[h, :, cols], s1.at[h, k], q1.at[h, k], mate)
        for k, (lo, hi) in enumerate(CUTS):
            multiply(h, k, 0)
            cols = pl.ds(lo, hi - lo)
            c1[h, k].wait()
            u[h, :, lo:hi] = part[0, h, :, lo:hi] + r1[h, :, lo:hi]
            c2[h, k] = send(u.at[h, :, cols], r2.at[h, :, cols], s2.at[h, k], q2.at[h, k], across)
            if (h, k) == LAST:
                direct.append(send(u.at[h, :, cols], v1, sv.at[0], qv.at[0], mate))
                direct.append(send(u.at[h, :, cols], v2, sv.at[1], qv.at[1], NSP - 1 - me))

    own(0, (0, 1))
    for c in wcopies:
        c.wait()
    far(0, (0,))
    gathered(0)
    product(0)
    own(1, (2,))
    far(0, (1,))
    far(1, (2,))
    gathered(1)
    product(1)
    for h in range(NH):
        for k, (lo, hi) in enumerate(CUTS):
            c2[h, k].wait()
            fin[h, :, lo:hi] = (u[h, :, lo:hi] + r2[h, :, lo:hi]).astype(jnp.bfloat16)
            cols = pl.ds(lo, hi - lo)
            if (h, k) != LAST:
                c3[h, k] = send(fin.at[h, :, cols], r3.at[h, :, cols], s3.at[h, k], q3.at[h, k], mate)
            out_ref[rows_of(h), pl.ds(pl.multiple_of(core * HALF + lo, HEAD), hi - lo)] = fin[h, :, lo:hi]
    for h in range(NH):
        for k, (lo, hi) in enumerate(CUTS):
            cols = pl.ds(pl.multiple_of((1 - core) * HALF + lo, HEAD), hi - lo)
            if (h, k) == LAST:
                for c in direct:
                    c.wait()
                out_ref[rows_of(h), cols] = (v1[...] + v2[...]).astype(jnp.bfloat16)
            else:
                c3[h, k].wait()
                out_ref[rows_of(h), cols] = r3[h, :, lo:hi]


def solution(mesh):
    row_spec = P(('rep', 'dp'), None)
    cache_spec = P(('rep', 'dp'), 'sp', None, None)
    len_spec = P(('rep', 'dp'))
    hbm = pl.BlockSpec(memory_space=pl.ANY)
    vmem = pl.BlockSpec(memory_space=pltpu.VMEM)
    smem = pl.BlockSpec(memory_space=pltpu.SMEM)
    bf16, f32, i32 = jnp.bfloat16, jnp.float32, jnp.int32
    dma = pltpu.SemaphoreType.DMA
    shaped = jax.ShapeDtypeStruct

    def local_step(hidden, w_query, w_key, w_value, w_out, k_cache, v_cache, write_pos, valid_len):
        kc = k_cache.reshape(ROWS, FLAT, HEAD)
        vc = v_cache.reshape(ROWS, FLAT, HEAD)
        pin = lambda x: pltpu.with_memory_space_constraint(x, pltpu.HBM)
        flat = shaped((ROWS, FLAT, HEAD), bf16)
        qs, new, cidx, kv, vv = pl.pallas_call(
            project_kernel,
            out_shape=[shaped((ROWS * 32, HEAD), f32), shaped((2, ROWS * 16, HEAD), f32), shaped((32, FLAT), i32), flat, flat],
            in_specs=[hbm] * 6,
            out_specs=[vmem] * 5,
            scratch_shapes=[
                pltpu.VMEM((ROWS, DIM), bf16), pltpu.VMEM((DIM, PW), bf16),
                pltpu.VMEM((ROWS, PW), bf16), pltpu.VMEM((NSP - 1, ROWS, PW), bf16),
                dma, dma((NP, 2)), dma((2, 2)), dma((NP, NSP - 1)), dma((NP, NSP - 1))],
            compiler_params=pltpu.CompilerParams(collective_id=0, has_side_effects=True, vmem_limit_bytes=14 << 20),
            name="project",
            cost_estimate=pl.CostEstimate(flops=10_000_000_000, bytes_accessed=34_000_000, transcendentals=0),
        )(pin(hidden), pin(w_query), pin(w_key), pin(w_value), pin(kc), pin(vc))
        tiles = (8, HEAD)
        k_new, v_new, kv, vv, acc, ml = pl.pallas_call(
            attend_kernel,
            out_shape=[flat, flat, flat, flat, shaped((KVH, EARLY) + tiles, f32), shaped((KVH, 2) + tiles, f32)],
            in_specs=[smem, smem] + [vmem] * 5,
            out_specs=[hbm, hbm, vmem, vmem, vmem, vmem],
            scratch_shapes=[dma((2, NE))],
            input_output_aliases={5: 2, 6: 3},
            compiler_params=pltpu.CompilerParams(vmem_limit_bytes=4 << 20),
            name="attend",
            cost_estimate=pl.CostEstimate(flops=7_000_000_000, bytes_accessed=34_000_000, transcendentals=0),
        )(write_pos, valid_len, qs, new, cidx, kv, vv)
        parts = (NH, HR, HALF)
        nx = len(CHUNKS)
        attn_out = pl.pallas_call(
            reduce_kernel,
            out_shape=shaped((ROWS, DIM), bf16),
            in_specs=[smem] + [vmem] * 6 + [hbm],
            out_specs=vmem,
            scratch_shapes=[
                pltpu.VMEM((KVH, LATE) + tiles, f32), pltpu.VMEM((KVH, 2) + tiles, f32),
                pltpu.VMEM((2, ROWS) + tiles, f32), pltpu.VMEM((2, 2, 2) + tiles, f32),
                pltpu.VMEM((ROWS,) + tiles, f32), pltpu.VMEM((2, 2) + tiles, f32),
                pltpu.VMEM((ROWS,) + tiles, f32), pltpu.VMEM((2, 2) + tiles, f32),
                pltpu.VMEM((ROWS * 8, HEAD), f32), pltpu.VMEM((NH, HR, QW), bf16), pltpu.VMEM((QW, DIM), bf16),
                pltpu.VMEM((2,) + parts, f32), pltpu.VMEM(parts, f32), pltpu.VMEM(parts, f32), pltpu.VMEM(parts, f32),
                pltpu.VMEM(parts, bf16), pltpu.VMEM(parts, bf16),
                dma((4,)), dma((nx, 2)), dma((nx, 2)), dma((2, 2)), dma((2, 2)), dma((nx,)), dma((nx,)), dma((2,)), dma((2,))]
                + [dma((NH, NC))] * 6
                + [pltpu.VMEM((HR, CUTS[-1][1] - CUTS[-1][0]), f32)] * 2 + [dma((2,))] * 2,
            compiler_params=pltpu.CompilerParams(collective_id=1, has_side_effects=True, vmem_limit_bytes=14 << 20),
            name="reduce",
            cost_estimate=pl.CostEstimate(flops=20_000_000_000, bytes_accessed=10_000_000, transcendentals=0),
        )(valid_len, qs, cidx, kv, vv, acc, ml, pin(w_out))
        shape = (ROWS, SEQ, KVH, HEAD)
        return attn_out, k_new.reshape(shape), v_new.reshape(shape)

    return jax.shard_map(local_step, mesh=mesh, in_specs=(row_spec, P(), P(), P(), P('sp', None), cache_spec, cache_spec, len_spec, len_spec), out_specs=(row_spec, cache_spec, cache_spec), check_vma=False)
```

```python
import jax
import jax.numpy as jnp
from jax import lax
from jax.experimental import pallas as pl
from jax.experimental.pallas import tpu as pltpu
from jax.sharding import PartitionSpec as P

MESH = pl.DeviceIdType.MESH
LOG2E = 1.4426950408889634
NSP = 4
ROWS = 32
DIM = 3584
HEAD = 128
KVH = 4
GRP = 7
SEQ = 256
FLAT = SEQ * KVH
QW = GRP * HEAD
PW = QW + 2 * HEAD
PIECES = ((0, 256), (256, 512), (512, 768), (768, QW), (QW, PW))
NP = len(PIECES)
OUT = (0, 8, 16, 24, 28, ROWS)
NE = len(OUT) - 1
EARLY = 24
LATE = ROWS - EARLY
NH = 2
HR = ROWS // NH
HALF = DIM // 2
CUTS = ((0, 512), (512, 1280), (1280, HALF))
NC = len(CUTS)
LAST = (NH - 1, NC - 1)
FACTOR = HEAD ** -0.5 * LOG2E
CHUNKS = ((0, HR), (HR, EARLY), (EARLY, ROWS))


def greet(me):
    barrier = pltpu.get_barrier_semaphore()
    for d in range(1, NSP):
        pl.semaphore_signal(barrier, inc=1, device_id={"sp": lax.rem(me + d, NSP)}, device_id_type=MESH)


def greeted():
    pl.semaphore_wait(pltpu.get_barrier_semaphore(), NSP - 1)


def send(src, dst, ssem, rsem, peer):
    c = pltpu.make_async_remote_copy(src_ref=src, dst_ref=dst, send_sem=ssem, recv_sem=rsem,
                                     device_id={"sp": peer}, device_id_type=MESH)
    c.start()
    return c


def project_kernel(h_ref, wq_ref, wk_ref, wv_ref, kc_ref, vc_ref, qs, new, cidx, ko_ref, vo_ref,
                   hbuf, wbuf, mine, recv, hsem, wsem, csem, ssem, rsem):
    me = lax.axis_index("sp")
    mate = me + 1 - 2 * lax.rem(me, 2)
    across = lax.rem(me + 2, NSP)
    qcol = pl.multiple_of(me * QW, HEAD)
    kcol = pl.multiple_of(me * HEAD, HEAD)
    hcopy = pltpu.make_async_copy(h_ref, hbuf, hsem)
    hcopy.start()
    copies = []
    for x, (lo, hi) in enumerate(PIECES):
        if hi <= QW:
            views = [(wq_ref.at[:, pl.ds(pl.multiple_of(qcol + lo, HEAD), hi - lo)], lo)]
        else:
            views = [(wk_ref.at[:, pl.ds(kcol, HEAD)], QW), (wv_ref.at[:, pl.ds(kcol, HEAD)], QW + HEAD)]
        some = []
        for y, (v, at) in enumerate(views):
            c = pltpu.make_async_copy(v, wbuf.at[:, pl.ds(at, v.shape[1])], wsem.at[x, y])
            c.start()
            some.append(c)
        copies.append(some)
    caches = []
    for j, (src, dst) in enumerate(((kc_ref, ko_ref), (vc_ref, vo_ref))):
        for i in range(2):
            part = pl.ds(i * (ROWS // 2), ROWS // 2)
            c = pltpu.make_async_copy(src.at[part], dst.at[part], csem.at[j, i])
            c.start(priority=1)
            caches.append(c)
    greet(me)
    col = lax.broadcasted_iota(jnp.int32, (32, FLAT), 1)
    head = lax.shift_right_logical(lax.broadcasted_iota(jnp.int32, (32, FLAT), 0), 3)
    cidx[...] = jnp.where(lax.bitwise_and(col, KVH - 1) == head, col, 1 << 20)
    for g in range(KVH):
        qs[pl.ds(g * 8 + GRP, ROWS, stride=32), :] = jnp.zeros((ROWS, HEAD), jnp.float32)
    hcopy.wait()
    peers = (across, NSP - 1 - me, mate)
    sends = []
    for x, (lo, hi) in enumerate(PIECES):
        for c in copies[x]:
            c.wait()
        mine[:, lo:hi] = jnp.dot(hbuf[...], wbuf[:, lo:hi], preferred_element_type=jnp.float32).astype(jnp.bfloat16)
        if x == 0:
            greeted()
        cols = pl.ds(lo, hi - lo)
        sends.append([send(mine.at[:, cols], recv.at[y, :, cols], ssem.at[x, y], rsem.at[x, y], peers[y]) for y in range(NSP - 1)])

    def place(g, x, read):
        lo, hi = PIECES[x]
        for at in range(lo, hi, HEAD):
            y = read(at).astype(jnp.float32)
            if at < QW:
                qs[pl.ds(g * 8 + at // HEAD, ROWS, stride=32), :] = y
            else:
                for r in range(4):
                    new[(at - QW) // HEAD, pl.ds(r * KVH + g, ROWS, stride=16), :] = y

    for x in range(NP):
        place(me, x, lambda at: mine[:, at:at + HEAD])
    for x in range(NP):
        for y in (2, 0, 1):
            sends[x][y].wait()
            place(peers[y], x, lambda at: recv[y, :, at:at + HEAD])
    for c in caches:
        c.wait()


def attention(first, count, unroll, rows0, len_ref, qs, cidx, k_ref, v_ref, acc, ml):
    base = lax.axis_index("sp") * SEQ
    lane = lax.broadcasted_iota(jnp.int32, (8, HEAD), 1)
    lowest = float(jnp.finfo(jnp.float32).min)

    def pair(p, carry):
        q0 = qs[pl.ds(pl.multiple_of(p * 64, 64), 32), :].astype(jnp.bfloat16)
        q1 = qs[pl.ds(pl.multiple_of(p * 64 + 32, 32), 32), :].astype(jnp.bfloat16)
        z = jnp.zeros((32, HEAD), jnp.bfloat16)
        lhs = jnp.concatenate([jnp.concatenate([q0, z], 1), jnp.concatenate([z, q1], 1)], 0)
        kk = jnp.concatenate([k_ref[2 * p], k_ref[2 * p + 1]], 1)
        s = lax.dot_general(lhs, kk, (((1,), (1,)), ((), ())), preferred_element_type=jnp.float32)
        ci = cidx[...]
        ws, ms, ls = [], [], []
        for i in range(2):
            lim = (len_ref[2 * p + i] - base) * KVH
            si = jnp.where(ci < lim, s[32 * i:32 * (i + 1)], -jnp.inf)
            m = jnp.maximum(jnp.max(si, axis=1, keepdims=True), lowest)
            w = jnp.exp2((si - m) * FACTOR)
            ls.append(jnp.sum(w, axis=1, keepdims=True))
            ms.append(m)
            ws.append(w.astype(jnp.bfloat16))
        vv = jnp.concatenate([v_ref[2 * p], v_ref[2 * p + 1]], 1)
        o = jnp.dot(jnp.concatenate(ws, 0), vv, preferred_element_type=jnp.float32)
        for i in range(2):
            b = 2 * p + i
            here = lane == b
            oi = o[32 * i:32 * (i + 1), HEAD * i:HEAD * (i + 1)]
            for g in range(KVH):
                acc[g, b - rows0] = oi[8 * g:8 * (g + 1)]
                ml[g, 0] = jnp.where(here, ms[i][8 * g:8 * (g + 1)], ml[g, 0])
                ml[g, 1] = jnp.where(here, ls[i][8 * g:8 * (g + 1)], ml[g, 1])
        return carry

    lax.fori_loop(first // 2, (first + count) // 2, pair, 0, unroll=unroll)


def attend_kernel(pos_ref, len_ref, qs, new, cidx, k_in, v_in, ko_ref, vo_ref, k_ref, v_ref, acc, ml, sem):
    del k_in, v_in
    base = lax.axis_index("sp") * SEQ
    row = lax.shift_right_logical(lax.broadcasted_iota(jnp.int32, (16, HEAD), 0), 2)

    def patch(first, last):
        todo = []
        for b in range(first, last):
            t = pos_ref[b] - base
            inside = jnp.logical_and(t >= 0, t < SEQ)
            tc = jnp.clip(t, 0, SEQ - 1)
            rows = pl.ds(pl.multiple_of(lax.shift_right_logical(tc, 2) * 16, 16), 16)
            sel = row == jnp.where(inside, lax.bitwise_and(tc, 3), -1)
            for j, ref in enumerate((k_ref, v_ref)):
                old = ref[b, rows, :].astype(jnp.float32)
                todo.append((ref, b, rows, jnp.where(sel, new[j, b * 16:(b + 1) * 16, :], old).astype(jnp.bfloat16)))
        for ref, b, rows, x in todo:
            ref[b, rows, :] = x

    copies = []
    for i in range(NE):
        lo, hi = OUT[i], OUT[i + 1]
        for b in range(lo, hi, 4):
            patch(b, b + 4)
        part = pl.ds(lo, hi - lo)
        for j, (src, dst) in enumerate(((k_ref, ko_ref), (v_ref, vo_ref))):
            c = pltpu.make_async_copy(src.at[part], dst.at[part], sem.at[j, i])
            c.start()
            copies.append(c)
    ml[:, 0] = jnp.zeros((KVH, 8, HEAD), jnp.float32)
    ml[:, 1] = jnp.ones((KVH, 8, HEAD), jnp.float32)
    attention(0, EARLY, EARLY // 2, 0, len_ref, qs, cidx, k_ref, v_ref, acc, ml)
    for c in copies:
        c.wait()


def combine(parts):
    top = parts[0][0]
    for m, _ in parts[1:]:
        top = jnp.maximum(top, m)
    ww = [jnp.exp2((m - top) * FACTOR) for m, _ in parts]
    total = ww[0] * parts[0][1]
    for w, (_, l) in zip(ww[1:], parts[1:]):
        total = total + w * l
    return top, total, ww


def reduce_kernel(len_ref, qs, cidx, k_ref, v_ref, acc0, ml0, wo_ref, out_ref,
                  acc1, ml1, ra, rma, cross, mcross, rb, rmb, osc, attn, wbuf, part, r1, u, r2, fin, r3,
                  wsem, sa, qa, sma, qma, sb, qb, smb, qmb, s1, q1, s2, q2, s3, q3, v1, v2, sv, qv):
    me = lax.axis_index("sp")
    core = lax.rem(me, 2)
    mate = me + 1 - 2 * core
    across = lax.rem(me + 2, NSP)
    greet(me)
    wcopies = []
    for i in range(4):
        rows = pl.ds(i * (QW // 4), QW // 4)
        c = pltpu.make_async_copy(wo_ref.at[rows], wbuf.at[rows], wsem.at[i])
        c.start(priority=1)
        wcopies.append(c)
    ml1[:, 0] = jnp.zeros((KVH, 8, HEAD), jnp.float32)
    ml1[:, 1] = jnp.ones((KVH, 8, HEAD), jnp.float32)
    greeted()

    theirs = (lax.rem(mate + 2, NSP), mate)
    mls = (ml0, ml1)
    accs = (acc0, acc1)
    starts = (0, EARLY)
    am, aa = {}, {}

    def to_mate(p, j, chunks):
        am[p, j] = send(mls[p].at[theirs[j]], rma.at[p, j], sma.at[p, j], qma.at[p, j], mate)
        for x in chunks:
            lo, hi = CHUNKS[x]
            aa[x, j] = send(accs[p].at[theirs[j], pl.ds(lo - starts[p], hi - lo)], ra.at[j, pl.ds(lo, hi - lo)],
                            sa.at[x, j], qa.at[x, j], mate)

    to_mate(0, 0, (0, 1))
    to_mate(0, 1, (0, 1))
    attention(EARLY, LATE // 2, LATE // 4, EARLY, len_ref, qs, cidx, k_ref, v_ref, acc1, ml1)
    bm, bb = {}, {}
    for p in range(2):
        if p == 1:
            attention(EARLY + LATE // 2, LATE // 2, LATE // 4, EARLY, len_ref, qs, cidx, k_ref, v_ref, acc1, ml1)
            to_mate(1, 0, (2,))
            to_mate(1, 1, (2,))
        am[p, 0].wait()
        top, total, ww = combine([(mls[p][across, 0], mls[p][across, 1]), (rma[p, 0, 0], rma[p, 0, 1])])
        mcross[p, 0] = top
        mcross[p, 1] = total
        bm[p] = send(mcross.at[p], rmb.at[p], smb.at[p], qmb.at[p], across)
        for x in ((0, 1), (2,))[p]:
            lo, hi = CHUNKS[x]
            aa[x, 0].wait()
            for b in range(lo, hi):
                cross[b] = accs[p][across, b - starts[p]] * ww[0][:, b:b + 1] + ra[0, b] * ww[1][:, b:b + 1]
            rows = pl.ds(lo, hi - lo)
            bb[x] = send(cross.at[rows], rb.at[rows], sb.at[x], qb.at[x], across)
    scales = {}

    def own(p, chunks):
        if p not in scales:
            am[p, 1].wait()
            bm[p].wait()
            _, total, ww = combine([(mls[p][me, 0], mls[p][me, 1]), (rma[p, 1, 0], rma[p, 1, 1]), (rmb[p, 0], rmb[p, 1])])
            inv = 1.0 / total
            scales[p] = [w * inv for w in ww]
        scale = scales[p]
        for x in chunks:
            aa[x, 1].wait()
            for b in range(*CHUNKS[x]):
                osc[pl.ds(b * 8, 8), :] = accs[p][me, b - starts[p]] * scale[0][:, b:b + 1] + ra[1, b] * scale[1][:, b:b + 1]

    def far(p, chunks):
        for x in chunks:
            bb[x].wait()
            for b in range(*CHUNKS[x]):
                osc[pl.ds(b * 8, 8), :] += rb[b] * scales[p][2][:, b:b + 1]

    def gathered(h):
        for j in range(GRP):
            attn[h, :, j * HEAD:(j + 1) * HEAD] = osc[pl.ds(h * HR * 8 + j, HR, stride=8), :].astype(jnp.bfloat16)

    c1, c2, c3, direct = {}, {}, {}, []
    rows_of = lambda h: pl.ds(h * HR, HR)

    def multiply(h, k, other):
        lo, hi = CUTS[k]
        half = lax.rem(core + other, 2)
        cols = pl.ds(pl.multiple_of(half * HALF + lo, HEAD), hi - lo)
        part[other, h, :, lo:hi] = jnp.dot(attn[h], wbuf[:, cols], preferred_element_type=jnp.float32)

    def product(h):
        for k, (lo, hi) in enumerate(CUTS):
            multiply(h, k, 1)
            cols = pl.ds(lo, hi - lo)
            c1[h, k] = send(part.at[1, h, :, cols], r1.at[h, :, cols], s1.at[h, k], q1.at[h, k], mate)
        for k, (lo, hi) in enumerate(CUTS):
            multiply(h, k, 0)
            cols = pl.ds(lo, hi - lo)
            c1[h, k].wait()
            u[h, :, lo:hi] = part[0, h, :, lo:hi] + r1[h, :, lo:hi]
            c2[h, k] = send(u.at[h, :, cols], r2.at[h, :, cols], s2.at[h, k], q2.at[h, k], across)
            if (h, k) == LAST:
                direct.append(send(u.at[h, :, cols], v1, sv.at[0], qv.at[0], mate))
                direct.append(send(u.at[h, :, cols], v2, sv.at[1], qv.at[1], NSP - 1 - me))

    own(0, (0, 1))
    for c in wcopies:
        c.wait()
    far(0, (0,))
    gathered(0)
    product(0)
    own(1, (2,))
    far(0, (1,))
    far(1, (2,))
    gathered(1)
    product(1)
    for h in range(NH):
        for k, (lo, hi) in enumerate(CUTS):
            c2[h, k].wait()
            fin[h, :, lo:hi] = (u[h, :, lo:hi] + r2[h, :, lo:hi]).astype(jnp.bfloat16)
            cols = pl.ds(lo, hi - lo)
            if (h, k) != LAST:
                c3[h, k] = send(fin.at[h, :, cols], r3.at[h, :, cols], s3.at[h, k], q3.at[h, k], mate)
            out_ref[rows_of(h), pl.ds(pl.multiple_of(core * HALF + lo, HEAD), hi - lo)] = fin[h, :, lo:hi]
    for h in range(NH):
        for k, (lo, hi) in enumerate(CUTS):
            cols = pl.ds(pl.multiple_of((1 - core) * HALF + lo, HEAD), hi - lo)
            if (h, k) == LAST:
                for c in direct:
                    c.wait()
                out_ref[rows_of(h), cols] = (v1[...] + v2[...]).astype(jnp.bfloat16)
            else:
                c3[h, k].wait()
                out_ref[rows_of(h), cols] = r3[h, :, lo:hi]


def solution(mesh):
    row_spec = P(('rep', 'dp'), None)
    cache_spec = P(('rep', 'dp'), 'sp', None, None)
    len_spec = P(('rep', 'dp'))
    hbm = pl.BlockSpec(memory_space=pl.ANY)
    vmem = pl.BlockSpec(memory_space=pltpu.VMEM)
    smem = pl.BlockSpec(memory_space=pltpu.SMEM)
    bf16, f32, i32 = jnp.bfloat16, jnp.float32, jnp.int32
    dma = pltpu.SemaphoreType.DMA
    shaped = jax.ShapeDtypeStruct

    def local_step(hidden, w_query, w_key, w_value, w_out, k_cache, v_cache, write_pos, valid_len):
        kc = k_cache.reshape(ROWS, FLAT, HEAD)
        vc = v_cache.reshape(ROWS, FLAT, HEAD)
        pin = lambda x: pltpu.with_memory_space_constraint(x, pltpu.HBM)
        flat = shaped((ROWS, FLAT, HEAD), bf16)
        qs, new, cidx, kv, vv = pl.pallas_call(
            project_kernel,
            out_shape=[shaped((ROWS * 32, HEAD), f32), shaped((2, ROWS * 16, HEAD), f32), shaped((32, FLAT), i32), flat, flat],
            in_specs=[hbm] * 6,
            out_specs=[vmem] * 5,
            scratch_shapes=[
                pltpu.VMEM((ROWS, DIM), bf16), pltpu.VMEM((DIM, PW), bf16),
                pltpu.VMEM((ROWS, PW), bf16), pltpu.VMEM((NSP - 1, ROWS, PW), bf16),
                dma, dma((NP, 2)), dma((2, 2)), dma((NP, NSP - 1)), dma((NP, NSP - 1))],
            compiler_params=pltpu.CompilerParams(collective_id=0, has_side_effects=True, vmem_limit_bytes=14 << 20),
            name="project",
            cost_estimate=pl.CostEstimate(flops=10_000_000_000, bytes_accessed=34_000_000, transcendentals=0),
        )(pin(hidden), pin(w_query), pin(w_key), pin(w_value), pin(kc), pin(vc))
        tiles = (8, HEAD)
        k_new, v_new, kv, vv, acc, ml = pl.pallas_call(
            attend_kernel,
            out_shape=[flat, flat, flat, flat, shaped((KVH, EARLY) + tiles, f32), shaped((KVH, 2) + tiles, f32)],
            in_specs=[smem, smem] + [vmem] * 5,
            out_specs=[hbm, hbm, vmem, vmem, vmem, vmem],
            scratch_shapes=[dma((2, NE))],
            input_output_aliases={5: 2, 6: 3},
            compiler_params=pltpu.CompilerParams(vmem_limit_bytes=4 << 20),
            name="attend",
            cost_estimate=pl.CostEstimate(flops=7_000_000_000, bytes_accessed=34_000_000, transcendentals=0),
        )(write_pos, valid_len, qs, new, cidx, kv, vv)
        parts = (NH, HR, HALF)
        nx = len(CHUNKS)
        attn_out = pl.pallas_call(
            reduce_kernel,
            out_shape=shaped((ROWS, DIM), bf16),
            in_specs=[smem] + [vmem] * 6 + [hbm],
            out_specs=vmem,
            scratch_shapes=[
                pltpu.VMEM((KVH, LATE) + tiles, f32), pltpu.VMEM((KVH, 2) + tiles, f32),
                pltpu.VMEM((2, ROWS) + tiles, f32), pltpu.VMEM((2, 2, 2) + tiles, f32),
                pltpu.VMEM((ROWS,) + tiles, f32), pltpu.VMEM((2, 2) + tiles, f32),
                pltpu.VMEM((ROWS,) + tiles, f32), pltpu.VMEM((2, 2) + tiles, f32),
                pltpu.VMEM((ROWS * 8, HEAD), f32), pltpu.VMEM((NH, HR, QW), bf16), pltpu.VMEM((QW, DIM), bf16),
                pltpu.VMEM((2,) + parts, f32), pltpu.VMEM(parts, f32), pltpu.VMEM(parts, f32), pltpu.VMEM(parts, f32),
                pltpu.VMEM(parts, bf16), pltpu.VMEM(parts, bf16),
                dma((4,)), dma((nx, 2)), dma((nx, 2)), dma((2, 2)), dma((2, 2)), dma((nx,)), dma((nx,)), dma((2,)), dma((2,))]
                + [dma((NH, NC))] * 6
                + [pltpu.VMEM((HR, CUTS[-1][1] - CUTS[-1][0]), f32)] * 2 + [dma((2,))] * 2,
            compiler_params=pltpu.CompilerParams(collective_id=1, has_side_effects=True, vmem_limit_bytes=14 << 20),
            name="reduce",
            cost_estimate=pl.CostEstimate(flops=20_000_000_000, bytes_accessed=10_000_000, transcendentals=0),
        )(valid_len, qs, cidx, kv, vv, acc, ml, pin(w_out))
        shape = (ROWS, SEQ, KVH, HEAD)
        return attn_out, k_new.reshape(shape), v_new.reshape(shape)

    return jax.shard_map(local_step, mesh=mesh, in_specs=(row_spec, P(), P(), P(), P('sp', None), cache_spec, cache_spec, len_spec, len_spec), out_specs=(row_spec, cache_spec, cache_spec), check_vma=False)
```
